128 devices in a mesh: key: 4 (over x_hi, core), head: 16 (over z, y), batch: 2 (over x_lo).
Axes of the slice: x: 4 (x_hi: 2, x_lo: 2; x = x_hi * 2 + x_lo), y: 4, z: 4, core: 2. Of those that a mesh axis runs over, the one named last changes fastest.
Arguments:
- new_queries: bfloat16 [16, 16, 4, 1024], P('batch', 'head'), parts along dimension 0, may hold values from -6 to 6
- new_keys: bfloat16 [16, 16, 4, 1024], P('batch', 'head'), parts along dimension 0, may hold values from -0.8984375 to 0.8984375
- new_values: bfloat16 [16, 16, 4, 1024], P('batch', 'head'), parts along dimension 0, may hold values from -6 to 6
- decay_gate: float32 [16, 16, 4], P('batch', 'head'), parts along dimension 0, may hold values from 0.85 to 0.999
- write_gate: float32 [16, 16, 4], P('batch', 'head'), parts along dimension 0, may hold values from 0.2 to 1
- ridge_shift: float32 [16], P('head'), may hold values from 0.5 to 2
- norm_gain: float32 [16, 1024], P('head', 'key'), may hold values from 0.1 to 1.9
- cov_state: bfloat16 [16, 16, 1024, 1024], P('batch', 'head', 'key'), parts along dimension 0, may hold values from -1 to 42, as said below
- value_state: bfloat16 [16, 16, 1024, 1024], P('batch', 'head', None, 'key'), parts along dimension 0, may hold values from -0.1875 to 0.1875
- out_weight: bfloat16 [16, 1024, 8192], P('head', 'key'), may hold values from -0.0625 to 0.0625
Outputs:
- layer_out: bfloat16 [16, 4, 8192], P('batch', None, ('key', 'head')), parts along dimension 0
The draws below stay inside these ranges and needn't reach their ends.
There are 2 independent parts, one for each index of `batch`. The reference program is written for one: setup_inputs(seed, part) draws one part's arguments, and reference() takes and returns one part's arrays. A program takes and returns all parts, laid end to end along the dimension named above; an argument that names none is the same for every part. Nothing has to cross between parts.
Inputs may be any that keep to these rules, and one draw needn't show every extreme that they name: `cov_state`: each 1024 x 1024 block is symmetric and positive definite.
All inputs are finite; a program needn't handle non-finite values.
Results may differ from the reference program's by a relative error of at most 0.0085.
Values may be sent and summed in bfloat16 or wider, within the bound.
No kernel may reach another device: no remote copies, remote signals or barrier semaphores. Data moves between devices by JAX's collectives and lax.ppermute only.
A program may use at most 64 MiB of HBM per device.

```python
import math
import jax
import jax.numpy as jnp
from jax import lax

DK = 1024
DV = 1024
DM = 8192
SEQS = 8
DRAFT = 4
ITERS = 3
HEADS = 16


def draw_cov_state(key, part):
    first_key, second_key = jax.random.split(jax.random.fold_in(key, 17))
    log_diag = jax.random.uniform(first_key, (SEQS, HEADS, DK), jnp.float32, math.log(2.0), math.log(20.0))
    noise = jax.random.normal(second_key, (SEQS, HEADS, DK, DK), jnp.float32)
    symmetric = (noise + jnp.swapaxes(noise, 2, 3)) * (0.02 / math.sqrt(2.0))
    diagonal = jnp.exp(log_diag)[..., None] * jnp.eye(DK, dtype=jnp.float32)
    return (symmetric + diagonal).astype(jnp.bfloat16)


def with_spikes(values, rng, source, target, blocks, factor):
    def block_of(axis_at):
        return (jnp.arange(values.shape[axis_at]) // (values.shape[axis_at] // blocks)).reshape((-1,) + (1,) * (values.ndim - 1 - axis_at))

    near = jax.random.permutation(rng, blocks)[block_of(target)]
    other_side = (block_of(target) + blocks // 2) % blocks
    return jnp.where((block_of(source) == near) | (block_of(source) == other_side), factor * values, values)


def block_levels(key, dims, cuts, least, largest):
    gain = 1.0
    for dim, blocks in cuts:
        draws = jax.random.uniform(jax.random.fold_in(jax.random.fold_in(key, 6), dim), (blocks,), jnp.float32, least / len(cuts), largest / len(cuts))
        gain = gain * jnp.repeat(jnp.exp(draws), dims[dim] // blocks).reshape((-1,) + (1,) * (len(dims) - 1 - dim))
    return gain


def bell_draw(rng, extent, deviation, most, cuts=(), held_as=jnp.bfloat16):
    gain = block_levels(rng, extent, cuts, -0.22, 0.18) if cuts else 1.0
    entries = jax.random.normal(rng, extent, jnp.float32) * deviation * gain
    return jnp.minimum(jnp.maximum(entries, -most), most).astype(held_as)


def heavy_noise(key, dims, spread, limit, shards, heavy, held_as=jnp.bfloat16):
    drawn = spread * jax.random.normal(key, dims, jnp.float32)
    if shards:
        drawn = drawn * block_levels(key, dims, shards, -0.22, 0.18)
    return jnp.clip(with_spikes(drawn, jax.random.fold_in(key, 3), *heavy), -limit, limit).astype(held_as)


def setup_inputs(seed: int = 0, part: int = 0) -> dict:
    streams_of = jax.random.split(jax.random.key(seed), 11)
    own_keys = jax.random.split(jax.random.fold_in(streams_of[10], part), 11)
    return {
        "new_queries": bell_draw(own_keys[0], (SEQS, HEADS, DRAFT, DK), 1.0, 6.0, ((1, 16),)),
        "new_keys": bell_draw(own_keys[1], (SEQS, HEADS, DRAFT, DK), 0.15, 0.8984375, ((1, 16),)),
        "new_values": bell_draw(own_keys[2], (SEQS, HEADS, DRAFT, DV), 1.0, 6.0, ((1, 16),)),
        "decay_gate": jnp.clip(jnp.exp(math.log(0.999) - 0.16151841 * jax.random.uniform(own_keys[3], (SEQS, HEADS, DRAFT), jnp.float32) ** block_levels(own_keys[3], (SEQS, HEADS, DRAFT), ((1, 16),), -0.2, 0.2)), 0.85, 0.999),
        "write_gate": jnp.clip(0.2 + 0.8 * jax.random.uniform(own_keys[4], (SEQS, HEADS, DRAFT), jnp.float32) ** block_levels(own_keys[4], (SEQS, HEADS, DRAFT), ((1, 16),), -0.2, 0.2), 0.2, 1.0),
        "ridge_shift": jnp.clip(jnp.exp(math.log(2.0) - 1.3862944 * jax.random.uniform(streams_of[5], (HEADS,), jnp.float32) ** block_levels(streams_of[5], (HEADS,), ((0, 16),), -0.2, 0.2)), 0.5, 2.0),
        "norm_gain": jnp.clip(1.0 + 0.18 * jax.random.normal(streams_of[6], (HEADS, DV), jnp.float32), 0.1, 1.9),
        "cov_state": draw_cov_state(jax.random.fold_in(jax.random.fold_in(streams_of[10], part), 71), part),
        "value_state": bell_draw(own_keys[8], (SEQS, HEADS, DV, DK), DK ** -0.5, 0.1875, ((1, 16), (3, 4))),
        "out_weight": heavy_noise(streams_of[9], (HEADS, DV, DM), (HEADS * DV) ** -0.5, 0.0625, ((0, 16), (1, 4)), (0, 2, 16, 2.0)),
    }


def coefficients(decay_gate, write_gate):
    decay_total = jnp.cumprod(decay_gate, axis=-1)
    decay_ratio = decay_total[..., :, None] / decay_total[..., None, :]
    is_later = jnp.arange(DRAFT)[:, None] >= jnp.arange(DRAFT)[None, :]
    mix_weights = jnp.where(is_later, write_gate[..., None, :] * decay_ratio, jnp.zeros_like(decay_ratio))
    return (decay_total, mix_weights)

def to_bf16_f32(vector):
    rounded = lax.optimization_barrier(vector.astype(jnp.bfloat16))
    return rounded.astype(jnp.float32)

def reference(new_queries, new_keys, new_values, decay_gate, write_gate, ridge_shift, norm_gain, cov_state, value_state, out_weight):
    high = lax.Precision.HIGHEST
    decay_total, mix_weights = coefficients(decay_gate, write_gate)
    keys_f = new_keys.astype(jnp.float32)
    values_f = new_values.astype(jnp.float32)
    cov_f = cov_state.astype(jnp.float32)
    ridge_term = ridge_shift[None, :, None, None]

    def operator(vector):
        vec_b = to_bf16_f32(vector)
        state_prod = jnp.einsum('shic,shtc->shti', cov_f, vec_b, precision=high)
        key_dots = jnp.einsum('shtc,shuc->shtu', vec_b, keys_f, precision=high)
        low_rank = jnp.einsum('shtu,shuc->shtc', mix_weights * key_dots, keys_f, precision=high)
        return decay_total[..., None] * state_prod + low_rank + ridge_term * vector
    residual = new_queries.astype(jnp.float32)
    direction = residual
    solution = jnp.zeros_like(residual)
    sq_norm = lax.optimization_barrier(jnp.sum(residual * residual, axis=-1))
    for sweep_index in range(ITERS):
        applied = operator(direction)
        step_size = sq_norm / lax.optimization_barrier(jnp.sum(direction * applied, axis=-1))
        solution = solution + step_size[..., None] * direction
        residual = residual - step_size[..., None] * applied
        new_norm = lax.optimization_barrier(jnp.sum(residual * residual, axis=-1))
        direction = residual + (new_norm / sq_norm)[..., None] * direction
        sq_norm = new_norm
    sol_b = to_bf16_f32(solution)
    state_read = jnp.einsum('shvc,shtc->shtv', value_state.astype(jnp.float32), sol_b, precision=high)
    key_sol = jnp.einsum('shtc,shuc->shtu', sol_b, keys_f, precision=high)
    readout = decay_total[..., None] * state_read + jnp.einsum('shtu,shuv->shtv', mix_weights * key_sol, values_f, precision=high)
    mean_sq = lax.optimization_barrier(jnp.mean(readout * readout, axis=-1))
    normed = (readout * lax.rsqrt(mean_sq + 1e-06)[..., None] * norm_gain[None, :, None, :]).astype(jnp.bfloat16)
    result = jnp.einsum('shtv,hvm->stm', normed.astype(jnp.float32), out_weight.astype(jnp.float32), precision=high)
    return result.astype(jnp.bfloat16)
```

```python
import functools

import jax
import jax.numpy as jnp
from jax import lax
from jax.experimental import pallas as pl
from jax.experimental.pallas import tpu as pltpu
from jax.sharding import Mesh, PartitionSpec as P

DRAFT = 4
SEQS = 8
ROWS = SEQS * DRAFT
DK = 1024
DV = 1024
PART = 256
HEADS = 16
F32 = jnp.float32
BF16 = jnp.bfloat16
KEY = ("xh", "core")
HBM = pl.BlockSpec(memory_space=pltpu.HBM)
VMEM = pl.BlockSpec(memory_space=pltpu.VMEM)
SMEM = pl.BlockSpec(memory_space=pltpu.SMEM)
NT = (((1,), (1,)), ((), ()))
NN = (((1,), (0,)), ((), ()))


def mm(a, b, dims=NN):
    return lax.dot_general(a, b, dims, preferred_element_type=F32)


def halves(x):
    hi = x.astype(BF16)
    return hi, (x - hi.astype(F32)).astype(BF16)


def mm_wide(a, b):
    hi, lo = halves(a)
    return mm(hi, b) + mm(lo, b)


def coefficients(decay, write):
    totals = [decay[0:1]]
    for t in range(1, DRAFT):
        totals.append(totals[-1] * decay[t : t + 1])
    row = lax.broadcasted_iota(jnp.int32, (ROWS, SEQS), 0)
    seq = lax.broadcasted_iota(jnp.int32, (ROWS, SEQS), 1)
    token = row % DRAFT

    def column(rows):
        spread = jnp.zeros((ROWS, SEQS), F32)
        for t in range(DRAFT):
            spread = jnp.where(token == t, jnp.broadcast_to(rows[t], (ROWS, SEQS)), spread)
        return jnp.sum(jnp.where(row // DRAFT == seq, spread, 0.0), axis=1, keepdims=True)

    total = column(totals)
    written = column([write[t : t + 1] for t in range(DRAFT)])
    i = lax.broadcasted_iota(jnp.int32, (ROWS, ROWS), 0)
    j = lax.broadcasted_iota(jnp.int32, (ROWS, ROWS), 1)

    def as_row(col):
        return jnp.sum(jnp.where(i == j, jnp.broadcast_to(col, (ROWS, ROWS)), 0.0), axis=0, keepdims=True)

    kept = (i // DRAFT == j // DRAFT) & (j <= i)
    mix = jnp.where(kept, as_row(written) * (total / as_row(total)), 0.0)
    return total, mix


def stack(ref, out):
    for s in range(SEQS):
        out[DRAFT * s : DRAFT * (s + 1), :] = ref[s].astype(F32)


def first_kernel(
    me, ridge, q_hbm, k_hbm, decay_hbm, write_hbm, cov_hbm, msg,
    q_in, k_in, decay_in, write_in, cov, q32, k32, z32, small_sem, cov_sem,
):
    small = [
        pltpu.make_async_copy(a, b, small_sem.at[n])
        for n, (a, b) in enumerate(
            [(q_hbm, q_in), (k_hbm, k_in), (decay_hbm, decay_in), (write_hbm, write_in)]
        )
    ]
    big = [pltpu.make_async_copy(cov_hbm.at[s], cov.at[s], cov_sem.at[s]) for s in range(SEQS)]
    for c in small + big:
        c.start()
    for c in small:
        c.wait()
    total, mix = coefficients(decay_in[...], write_in[...])
    stack(q_in, q32)
    stack(k_in, k32)
    start = pl.multiple_of(me[0] * PART, PART)
    keys = k32[...].astype(BF16)
    keys_mine = k32[:, pl.ds(start, PART)].astype(BF16)
    dots = mm(q32[...].astype(BF16), keys, NT)
    base = mm_wide(mix * dots, keys_mine) + ridge[0] * q32[:, pl.ds(start, PART)]
    first = lax.broadcasted_iota(jnp.int32, (8, 1), 0) < DRAFT

    def by_columns(p, pieces):
        both = jnp.concatenate(pieces, axis=0)
        res = [mm(both, cov[2 * p + n]) for n in range(2)]
        z = jnp.where(first, res[0][:8] + res[0][8:], res[1][:8] + res[1][8:])
        z32[8 * p : 8 * p + 8, :] = z * total[8 * p : 8 * p + 8]

    held = None
    for p in range(SEQS // 2):
        big[2 * p].wait()
        big[2 * p + 1].wait()
        slab = q32[8 * p : 8 * p + 8, :].astype(BF16)
        res = [mm(slab, cov[2 * p + n], NT) for n in range(2)]
        y = jnp.where(first, res[0], res[1]) * total[8 * p : 8 * p + 8] + base[8 * p : 8 * p + 8]
        pieces = halves(y)
        msg[8 * p : 8 * p + 8, DK : DK + PART] = pieces[0]
        msg[8 * p : 8 * p + 8, DK + PART :] = pieces[1]
        if held is not None:
            by_columns(*held)
        held = (p, pieces)
    by_columns(*held)
    y_hi, y_lo = msg[:, DK : DK + PART], msg[:, DK + PART :]
    dots = mm(y_hi, keys_mine, NT) + mm(y_lo, keys_mine, NT)
    msg[:, :DK] = (z32[...] + mm_wide(mix * dots, keys)).astype(BF16)


def second_kernel(
    me, ridge, gathered, q_in, k_in, v_in, decay_in, write_in, cov, val, sent, kept,
    q32, k32, v32, d32, x32, r1, r2, quad32,
):
    total, mix = coefficients(decay_in[...], write_in[...])
    stack(q_in, q32)
    stack(k_in, k32)
    stack(v_in, v32)
    start = pl.multiple_of(me[0] * PART, PART)
    core, xh = me[1], me[2]

    def dot(a, b):
        return jnp.sum(a * b, axis=1, keepdims=True)

    q = q32[...]
    y = jnp.concatenate(
        [
            gathered[g, :, DK : DK + PART].astype(F32) + gathered[g, :, DK + PART :].astype(F32)
            for g in range(4)
        ],
        axis=1,
    )
    w = ridge[0] * y
    for g in range(4):
        w = w + gathered[g, :, :DK].astype(F32)
    rr0 = dot(q, q)
    a0 = rr0 / dot(q, y)
    res1 = q - a0 * y
    rr1 = dot(res1, res1)
    b0 = rr1 / rr0
    dir1 = res1 + b0 * q
    image = (1.0 + b0) * y - a0 * w
    a1 = rr1 / dot(dir1, image)
    sol2 = a0 * q + a1 * dir1
    res2 = res1 - a1 * image
    rr2 = dot(res2, res2)
    dir2 = res2 + (rr2 / rr1) * dir1
    d32[...] = dir2
    x32[...] = sol2
    keys = k32[...].astype(BF16)
    d_bf, x_bf = dir2.astype(BF16), sol2.astype(BF16)
    dots_d = mm(d_bf, keys, NT)
    dots_x = mm(x_bf, keys, NT)
    local = jnp.sum(mix * dots_d * dots_d, axis=1, keepdims=True) + ridge[0] * dot(dir2, dir2)
    first = lax.broadcasted_iota(jnp.int32, (8, 1), 0) < DRAFT
    for p in range(SEQS // 2):
        rows = slice(8 * p, 8 * p + 8)
        lhs = jnp.concatenate(halves(d32[rows, :]), axis=0)
        res = [mm(lhs, cov[2 * p + n], NT) for n in range(2)]
        t = jnp.where(first, res[0][:8] + res[0][8:], res[1][:8] + res[1][8:])
        quad32[rows, :] = t * d32[rows, pl.ds(start, PART)]
    for p in range(SEQS // 2):
        rows = slice(8 * p, 8 * p + 8)
        lhs = jnp.concatenate(
            [x32[rows, pl.ds(start, PART)].astype(BF16), d32[rows, pl.ds(start, PART)].astype(BF16)], axis=0
        )
        res = [mm(lhs, val[2 * p + n], NT) for n in range(2)]
        r1[rows, :] = jnp.where(first, res[0][:8], res[1][:8]) * total[rows]
        r2[rows, :] = jnp.where(first, res[0][8:], res[1][8:]) * total[rows]
    values = v32[:, pl.ds(start, PART)].astype(BF16)
    r1[:, pl.ds(start, PART)] += mm_wide(mix * dots_x, values)
    r2[:, pl.ds(start, PART)] += mm_wide(mix * dots_d, values)
    share = (total * jnp.sum(quad32[...], axis=1, keepdims=True) + 0.25 * local) / rr2
    share = jnp.broadcast_to(share, (ROWS, 128))
    for out, c in ((sent, 1 - core), (kept, core)):
        for x in range(2):
            cols = pl.ds(pl.multiple_of((2 * x + c) * PART, PART), PART)
            out[:, x * PART : (x + 1) * PART] = r1[:, cols].astype(out.dtype)
            out[:, (2 + x) * PART : (3 + x) * PART] = r2[:, cols].astype(out.dtype)
        out[:, 4 * PART :] = share.astype(out.dtype)


def third_kernel(me, mine, arrived, gain, weight, sent, kept):
    core, xh = me[1], me[2]
    total = mine[...].astype(F32) + arrived[...].astype(F32)
    a2 = 1.0 / total[:, 4 * PART : 4 * PART + 1]
    readout = total[:, : 2 * PART] + a2 * total[:, 2 * PART : 4 * PART]
    squares = jnp.broadcast_to(jnp.sum(readout * readout, axis=1, keepdims=True), (ROWS, 128))
    own = jnp.where(xh == 0, readout[:, :PART], readout[:, PART:])
    scaled = (own * gain[...]).astype(BF16)
    step = 512
    for out, c in ((sent, 1 - core), (kept, core)):
        for x in range(2):
            for n in range(2048 // step):
                cols = pl.ds(pl.multiple_of((2 * x + c) * 2048 + n * step, step), step)
                part = mm(scaled, weight[:, cols])
                for m in range(step // 128):
                    out[16 * x + n * (step // 128) + m] = part[:, 128 * m : 128 * (m + 1)].astype(out.dtype)
        hi, lo = halves(squares)
        out[32] = hi.astype(out.dtype)
        out[33] = lo.astype(out.dtype)


def swapped(x, axis):
    return lax.ppermute(x, axis, [(0, 1), (1, 0)])


def params(mib):
    return pltpu.CompilerParams(vmem_limit_bytes=mib << 20)


def body(
    new_queries, new_keys, new_values, decay_gate, write_gate,
    ridge_shift, norm_gain, cov_state, value_state, out_weight,
):
    xh, core = lax.axis_index("xh"), lax.axis_index("core")
    me = jnp.stack([2 * xh + core, core, xh]).astype(jnp.int32)
    q, k, v = (x[:, 0] for x in (new_queries, new_keys, new_values))
    decay, write = (x[:, 0].T for x in (decay_gate, write_gate))
    cov, val, weight = cov_state[:, 0], value_state[:, 0], out_weight[0]

    msg = pl.pallas_call(
        first_kernel,
        name="first",
        out_shape=jax.ShapeDtypeStruct((ROWS, DK + 2 * PART), BF16),
        in_specs=[SMEM, SMEM] + [HBM] * 5,
        out_specs=VMEM,
        scratch_shapes=[
            pltpu.VMEM((SEQS, DRAFT, DK), BF16),
            pltpu.VMEM((SEQS, DRAFT, DK), BF16),
            pltpu.VMEM((DRAFT, SEQS), F32),
            pltpu.VMEM((DRAFT, SEQS), F32),
            pltpu.VMEM((SEQS, PART, DK), BF16),
            pltpu.VMEM((ROWS, DK), F32),
            pltpu.VMEM((ROWS, DK), F32),
            pltpu.VMEM((ROWS, DK), F32),
            pltpu.SemaphoreType.DMA((4,)),
            pltpu.SemaphoreType.DMA((SEQS,)),
        ],
        compiler_params=params(16),
    )(me, ridge_shift, q, k, decay, write, cov)
    gathered = lax.all_gather(msg, KEY)
    sent, kept = pl.pallas_call(
        second_kernel,
        name="second",
        out_shape=(
            jax.ShapeDtypeStruct((ROWS, 4 * PART + 128), BF16),
            jax.ShapeDtypeStruct((ROWS, 4 * PART + 128), F32),
        ),
        in_specs=[SMEM, SMEM] + [VMEM] * 8,
        out_specs=(VMEM, VMEM),
        scratch_shapes=[pltpu.VMEM((ROWS, DK), F32) for _ in range(7)] + [pltpu.VMEM((ROWS, PART), F32)],
        compiler_params=params(24),
    )(me, ridge_shift, gathered, q, k, v, decay, write, cov, val)
    pair = (kept + swapped(sent, "core").astype(F32)).astype(BF16)
    other = swapped(pair, "xh")
    sent, kept = pl.pallas_call(
        third_kernel,
        name="third",
        out_shape=(
            jax.ShapeDtypeStruct((34, ROWS, 128), BF16),
            jax.ShapeDtypeStruct((34, ROWS, 128), F32),
        ),
        in_specs=[SMEM] + [VMEM] * 4,
        out_specs=(VMEM, VMEM),
        compiler_params=params(24),
    )(me, pair, other, norm_gain, weight)
    arrived = swapped(sent, "core").astype(F32)
    squares = kept[32] + kept[33] + arrived[32] + arrived[33]
    scale = lax.rsqrt(squares * (1.0 / DV) + 1e-06)
    part = ((kept[:32] + arrived[:32]) * scale).astype(BF16)
    landed = lax.all_to_all(part, ("xh", "head"), 0, 0, tiled=True)
    out = landed.astype(F32).sum(axis=0).astype(BF16)
    return out.reshape(SEQS, DRAFT, 128)


def solution(mesh):
    fine = Mesh(mesh.devices.reshape(2, 2, *mesh.devices.shape[1:]), ("xh", "core", "head", "batch"))
    placed = (
        P("batch", "head", None, None),
        P("batch", "head", None, None),
        P("batch", "head", None, None),
        P("batch", "head", None),
        P("batch", "head", None),
        P("head"),
        P("head", KEY),
        P("batch", "head", KEY, None),
        P("batch", "head", None, KEY),
        P("head", KEY, None),
    )
    return jax.shard_map(
        body,
        mesh=fine,
        in_specs=placed,
        out_specs=P("batch", None, ("xh", "core", "head")),
        check_vma=False,
    )
```

```python
import jax
import jax.numpy as jnp
from jax import lax
from jax.experimental import pallas as pl
from jax.experimental.pallas import tpu as pltpu
from jax.sharding import Mesh, PartitionSpec as P

DRAFT = 4
SEQS = 8
ROWS = SEQS * DRAFT
DK = 1024
DV = 1024
PART = 256
HEADS = 16
F32 = jnp.float32
BF16 = jnp.bfloat16
KEY = ("xh", "core")
HBM = pl.BlockSpec(memory_space=pltpu.HBM)
VMEM = pl.BlockSpec(memory_space=pltpu.VMEM)
NT = (((1,), (1,)), ((), ()))
NN = (((1,), (0,)), ((), ()))


def mm(a, b, dims=NN):
    return lax.dot_general(a, b, dims, preferred_element_type=F32)


def halves(x):
    hi = x.astype(BF16)
    return hi, (x - hi.astype(F32)).astype(BF16)


def mm_wide(a, b):
    hi, lo = halves(a)
    return mm(hi, b) + mm(lo, b)


def coefficients(decay, write):
    totals = [decay[0:1]]
    for t in range(1, DRAFT):
        totals.append(totals[-1] * decay[t : t + 1])
    row = lax.broadcasted_iota(jnp.int32, (ROWS, SEQS), 0)
    seq = lax.broadcasted_iota(jnp.int32, (ROWS, SEQS), 1)
    token = row % DRAFT

    def column(rows):
        spread = jnp.zeros((ROWS, SEQS), F32)
        for t in range(DRAFT):
            spread = jnp.where(token == t, jnp.broadcast_to(rows[t], (ROWS, SEQS)), spread)
        return jnp.sum(jnp.where(row // DRAFT == seq, spread, 0.0), axis=1, keepdims=True)

    total = column(totals)
    written = column([write[t : t + 1] for t in range(DRAFT)])
    i = lax.broadcasted_iota(jnp.int32, (ROWS, ROWS), 0)
    j = lax.broadcasted_iota(jnp.int32, (ROWS, ROWS), 1)

    def as_row(col):
        return jnp.sum(jnp.where(i == j, jnp.broadcast_to(col, (ROWS, ROWS)), 0.0), axis=0, keepdims=True)

    kept = (i // DRAFT == j // DRAFT) & (j <= i)
    mix = jnp.where(kept, as_row(written) * (total / as_row(total)), 0.0)
    return total, mix


def stack(ref, out):
    for s in range(SEQS):
        out[DRAFT * s : DRAFT * (s + 1), :] = ref[s].astype(F32)


def position():
    xh, core = lax.axis_index("xh"), lax.axis_index("core")
    return 2 * xh + core, core, xh


def first_kernel(
    q_hbm, k_hbm, v_hbm, decay_hbm, write_hbm, cov_hbm, val_hbm,
    msg, cov, val, q32, k32, v_mine, total_out, mix_out,
    q_in, k_in, v_in, decay_in, write_in, z32, small_sem, big_sem,
):
    start = pl.multiple_of(position()[0] * PART, PART)
    ends = [
        (decay_hbm, decay_in),
        (write_hbm, write_in),
        (q_hbm, q_in),
        (k_hbm, k_in),
        (v_hbm.at[:, :, pl.ds(start, PART)], v_in),
    ]
    small = [pltpu.make_async_copy(a, b, small_sem.at[n]) for n, (a, b) in enumerate(ends)]
    big = [
        pltpu.make_async_copy(cov_hbm.at[pl.ds(2 * p, 2)], cov.at[pl.ds(2 * p, 2)], big_sem.at[p])
        for p in range(SEQS // 2)
    ]
    big.append(pltpu.make_async_copy(val_hbm, val, big_sem.at[SEQS // 2]))
    for c in small + big[:1]:
        c.start()
    for c in small[:2]:
        c.wait()
    big[1].start()
    big[2].start()
    total, mix = coefficients(decay_in[...], write_in[...])
    total_out[...] = jnp.broadcast_to(total, total_out.shape)
    mix_out[...] = mix
    for c, x, out in zip(small[2:], (q_in, k_in, v_in), (q32, k32, v_mine)):
        c.wait()
        stack(x, out)
    keys = k32[...].astype(BF16)
    keys_mine = k32[:, pl.ds(start, PART)].astype(BF16)
    dots = mm(q32[...].astype(BF16), keys, NT)
    base = mm_wide(mix * dots, keys_mine)
    first = lax.broadcasted_iota(jnp.int32, (8, 1), 0) < DRAFT

    def by_columns(p, pieces):
        both = jnp.concatenate(pieces, axis=0)
        res = [mm(both, cov[2 * p + n]) for n in range(2)]
        z = jnp.where(first, res[0][:8] + res[0][8:], res[1][:8] + res[1][8:])
        z32[8 * p : 8 * p + 8, :] = z * total[8 * p : 8 * p + 8]

    held = None
    for p in range(SEQS // 2):
        big[p].wait()
        if p == 0:
            big[3].start()
            big[4].start()
        slab = q32[8 * p : 8 * p + 8, :].astype(BF16)
        res = [mm(slab, cov[2 * p + n], NT) for n in range(2)]
        y = jnp.where(first, res[0], res[1]) * total[8 * p : 8 * p + 8] + base[8 * p : 8 * p + 8]
        pieces = halves(y)
        msg[8 * p : 8 * p + 8, DK : DK + PART] = pieces[0]
        msg[8 * p : 8 * p + 8, DK + PART :] = pieces[1]
        if held is not None:
            by_columns(*held)
        held = (p, pieces)
    by_columns(*held)
    y_hi, y_lo = msg[:, DK : DK + PART], msg[:, DK + PART :]
    dots = mm(y_hi, keys_mine, NT) + mm(y_lo, keys_mine, NT)
    msg[:, :DK] = (z32[...] + mm_wide(mix * dots, keys)).astype(BF16)
    big[4].wait()


def second_kernel(
    ridge, gathered, cov, val, q32, k32, v_mine, total_in, mix_in, sent, kept,
    y32, w32, d32, x32, aw32, r1, r2, l1, l2,
):
    total, shift, mix = total_in[:, :1], ridge[0:1, 0:1], mix_in[...]
    me, core, _ = position()
    mine = pl.ds(pl.multiple_of(me * PART, PART), PART)
    first = lax.broadcasted_iota(jnp.int32, (8, 1), 0) < DRAFT

    def dot(a, b):
        return jnp.sum(a * b, axis=1, keepdims=True)

    for g in range(4):
        y32[:, g * PART : (g + 1) * PART] = gathered[g, :, DK : DK + PART].astype(F32) + gathered[
            g, :, DK + PART :
        ].astype(F32)
    w = y32[...]
    y32[...] = w + shift * q32[...]
    w = shift * (w + y32[...])
    for g in range(4):
        w = w + gathered[g, :, :DK].astype(F32)
    w32[...] = w
    keys = k32[...].astype(BF16)
    keys_mine = k32[:, mine].astype(BF16)
    for p in range(SEQS // 2):
        rows = slice(8 * p, 8 * p + 8)
        lhs = jnp.concatenate(halves(w32[rows, :]), axis=0)
        res = [mm(lhs, cov[2 * p + n], NT) for n in range(2)]
        aw32[rows, :] = jnp.where(first, res[0][:8] + res[0][8:], res[1][:8] + res[1][8:]) * total[rows]
    dots_w = mm(jnp.concatenate(halves(w32[...]), axis=0), keys, NT)
    image_w = aw32[...] + mm_wide(mix * (dots_w[:ROWS] + dots_w[ROWS:]), keys_mine) + shift * w32[:, mine]

    q, y, w = q32[...], y32[...], w32[...]
    rr0 = dot(q, q)
    a0 = rr0 / dot(q, y)
    res1 = q - a0 * y
    rr1 = dot(res1, res1)
    b0 = rr1 / rr0
    dir1 = res1 + b0 * q
    image1 = (1.0 + b0) * y - a0 * w
    a1 = rr1 / dot(dir1, image1)
    sol2 = a0 * q + a1 * dir1
    res2 = res1 - a1 * image1
    rr2 = dot(res2, res2)
    b1 = rr2 / rr1
    dir2 = res2 + b1 * dir1
    d32[...] = dir2
    x32[...] = sol2
    y, w = y32[:, mine], w32[:, mine]
    image2 = y - a0 * w - a1 * ((1.0 + b0) * w - a0 * image_w) + b1 * ((1.0 + b0) * y - a0 * w)
    share = jnp.broadcast_to(dot(d32[:, mine], image2) / rr2, (ROWS, 128))
    dots = mm(jnp.concatenate(halves(sol2) + (dir2.astype(BF16),), axis=0), keys, NT)
    values = v_mine[...].astype(BF16)
    l1[...] = mm_wide(mix * (dots[:ROWS] + dots[ROWS : 2 * ROWS]), values)
    l2[...] = mm_wide(mix * dots[2 * ROWS :], values)
    for out in (sent, kept):
        out[:, 4 * PART :] = share.astype(out.dtype)
    for p in range(SEQS // 2):
        rows = slice(8 * p, 8 * p + 8)
        lhs = jnp.concatenate([x32[rows, mine].astype(BF16), d32[rows, mine].astype(BF16)], axis=0)
        res = [mm(lhs, val[2 * p + n], NT) for n in range(2)]
        r1[rows, :] = jnp.where(first, res[0][:8], res[1][:8]) * total[rows]
        r2[rows, :] = jnp.where(first, res[0][8:], res[1][8:]) * total[rows]
        r1[rows, mine] += l1[rows, :]
        r2[rows, mine] += l2[rows, :]
        for out, c in ((sent, 1 - core), (kept, core)):
            for x in range(2):
                cols = pl.ds(pl.multiple_of((2 * x + c) * PART, PART), PART)
                out[rows, x * PART : (x + 1) * PART] = r1[rows, cols].astype(out.dtype)
                out[rows, (2 + x) * PART : (3 + x) * PART] = r2[rows, cols].astype(out.dtype)


def third_kernel(mine, arrived, gain, weight, sent, kept):
    _, core, xh = position()
    total = mine[...].astype(F32) + arrived[...].astype(F32)
    a2 = 1.0 / total[:, 4 * PART : 4 * PART + 1]
    readout = total[:, : 2 * PART] + a2 * total[:, 2 * PART : 4 * PART]
    squares = jnp.broadcast_to(jnp.sum(readout * readout, axis=1, keepdims=True), (ROWS, 128))
    own = jnp.where(xh == 0, readout[:, :PART], readout[:, PART:])
    scaled = (own * gain[...]).astype(BF16)
    step = 512
    for out, c in ((sent, 1 - core), (kept, core)):
        for x in range(2):
            for n in range(2048 // step):
                cols = pl.ds(pl.multiple_of((2 * x + c) * 2048 + n * step, step), step)
                part = mm(scaled, weight[:, cols])
                for m in range(step // 128):
                    out[16 * x + n * (step // 128) + m] = part[:, 128 * m : 128 * (m + 1)].astype(out.dtype)
        hi, lo = halves(squares)
        out[32] = hi.astype(out.dtype)
        out[33] = lo.astype(out.dtype)


def swapped(x, axis):
    return lax.ppermute(x, axis, [(0, 1), (1, 0)])


def params(mib):
    return pltpu.CompilerParams(vmem_limit_bytes=mib << 20)


def body(
    new_queries, new_keys, new_values, decay_gate, write_gate,
    ridge_shift, norm_gain, cov_state, value_state, out_weight,
):
    q, k, v = (x[:, 0] for x in (new_queries, new_keys, new_values))
    decay, write = (x[:, 0].T for x in (decay_gate, write_gate))
    cov, val, weight = cov_state[:, 0], value_state[:, 0], out_weight[0]

    in_hbm = [
        pltpu.with_memory_space_constraint(x, pltpu.HBM)
        for x in (q, k, v, decay, write, cov, val)
    ]
    msg, *carried = pl.pallas_call(
        first_kernel,
        name="first",
        out_shape=(
            pltpu.VMEM((ROWS, DK + 2 * PART), BF16),
            pltpu.VMEM((SEQS, PART, DK), BF16),
            pltpu.VMEM((SEQS, DV, PART), BF16),
            pltpu.VMEM((ROWS, DK), F32),
            pltpu.VMEM((ROWS, DK), F32),
            pltpu.VMEM((ROWS, PART), F32),
            pltpu.VMEM((ROWS, 128), F32),
            pltpu.VMEM((ROWS, ROWS), F32),
        ),
        in_specs=[HBM] * 7,
        out_specs=(VMEM,) * 8,
        scratch_shapes=[
            pltpu.VMEM((SEQS, DRAFT, DK), BF16),
            pltpu.VMEM((SEQS, DRAFT, DK), BF16),
            pltpu.VMEM((SEQS, DRAFT, PART), BF16),
            pltpu.VMEM((DRAFT, SEQS), F32),
            pltpu.VMEM((DRAFT, SEQS), F32),
            pltpu.VMEM((ROWS, DK), F32),
            pltpu.SemaphoreType.DMA((5,)),
            pltpu.SemaphoreType.DMA((SEQS // 2 + 1,)),
        ],
        compiler_params=params(16),
    )(*in_hbm)
    gathered = lax.all_gather(msg, KEY)
    sent, kept = pl.pallas_call(
        second_kernel,
        name="second",
        out_shape=(
            jax.ShapeDtypeStruct((ROWS, 4 * PART + 128), BF16),
            jax.ShapeDtypeStruct((ROWS, 4 * PART + 128), F32),
        ),
        in_specs=[VMEM] * 9,
        out_specs=(VMEM, VMEM),
        scratch_shapes=[pltpu.VMEM((ROWS, n), F32) for n in (DK, DK, DK, DK, PART, DV, DV, PART, PART)],
        compiler_params=params(16),
    )(jnp.broadcast_to(ridge_shift[None], (8, 128)), gathered, *carried)
    pair = (kept + swapped(sent, "core").astype(F32)).astype(BF16)
    other = swapped(pair, "xh")
    sent, kept = pl.pallas_call(
        third_kernel,
        name="third",
        out_shape=(
            jax.ShapeDtypeStruct((34, ROWS, 128), BF16),
            jax.ShapeDtypeStruct((34, ROWS, 128), F32),
        ),
        in_specs=[VMEM] * 4,
        out_specs=(VMEM, VMEM),
        compiler_params=params(16),
    )(pair, other, norm_gain, weight)
    arrived = swapped(sent, "core").astype(F32)
    squares = kept[32] + kept[33] + arrived[32] + arrived[33]
    scale = lax.rsqrt(squares * (1.0 / DV) + 1e-06)
    part = ((kept[:32] + arrived[:32]) * scale).astype(BF16)
    landed = lax.all_to_all(part, ("xh", "head"), 0, 0, tiled=True)
    out = landed.astype(F32).sum(axis=0).astype(BF16)
    return out.reshape(SEQS, DRAFT, 128)


def solution(mesh):
    fine = Mesh(mesh.devices.reshape(2, 2, *mesh.devices.shape[1:]), ("xh", "core", "head", "batch"))
    placed = (
        P("batch", "head", None, None),
        P("batch", "head", None, None),
        P("batch", "head", None, None),
        P("batch", "head", None),
        P("batch", "head", None),
        P("head"),
        P("head", KEY),
        P("batch", "head", KEY, None),
        P("batch", "head", None, KEY),
        P("head", KEY, None),
    )
    return jax.shard_map(
        body,
        mesh=fine,
        in_specs=placed,
        out_specs=P("batch", None, ("xh", "core", "head")),
        check_vma=False,
    )
```

```python
import jax
import jax.numpy as jnp
from jax import lax
from jax.experimental import pallas as pl
from jax.experimental.pallas import tpu as pltpu
from jax.sharding import Mesh, PartitionSpec as P

DRAFT = 4
SEQS = 8
ROWS = SEQS * DRAFT
DK = 1024
DV = 1024
PART = 256
BLOCKS = DK // PART
HEADS = 16
F32 = jnp.float32
BF16 = jnp.bfloat16
KEY = ("xh", "core")
HBM = pl.BlockSpec(memory_space=pltpu.HBM)
VMEM = pl.BlockSpec(memory_space=pltpu.VMEM)
NT = (((1,), (1,)), ((), ()))
NN = (((1,), (0,)), ((), ()))


def mm(a, b, dims=NN):
    return lax.dot_general(a, b, dims, preferred_element_type=F32)


def halves(x):
    hi = x.astype(BF16)
    return hi, (x - hi.astype(F32)).astype(BF16)


def mm_wide(a, b):
    hi, lo = halves(a)
    return mm(hi, b) + mm(lo, b)


def by_rows(a, cov, s):
    return sum(mm(a[:, PART * b : PART * (b + 1)], cov[s, b], NT) for b in range(BLOCKS))


def coefficients(decay, write):
    totals = [decay[0:1]]
    for t in range(1, DRAFT):
        totals.append(totals[-1] * decay[t : t + 1])
    row = lax.broadcasted_iota(jnp.int32, (ROWS, SEQS), 0)
    seq = lax.broadcasted_iota(jnp.int32, (ROWS, SEQS), 1)
    token = row % DRAFT

    def column(rows):
        spread = jnp.zeros((ROWS, SEQS), F32)
        for t in range(DRAFT):
            spread = jnp.where(token == t, jnp.broadcast_to(rows[t], (ROWS, SEQS)), spread)
        return jnp.sum(jnp.where(row // DRAFT == seq, spread, 0.0), axis=1, keepdims=True)

    total = column(totals)
    written = column([write[t : t + 1] for t in range(DRAFT)])
    i = lax.broadcasted_iota(jnp.int32, (ROWS, ROWS), 0)
    j = lax.broadcasted_iota(jnp.int32, (ROWS, ROWS), 1)

    def as_row(col):
        return jnp.sum(jnp.where(i == j, jnp.broadcast_to(col, (ROWS, ROWS)), 0.0), axis=0, keepdims=True)

    kept = (i // DRAFT == j // DRAFT) & (j <= i)
    mix = jnp.where(kept, as_row(written) * (total / as_row(total)), 0.0)
    return total, mix


def stack(ref, out):
    for s in range(SEQS):
        out[DRAFT * s : DRAFT * (s + 1), :] = ref[s].astype(F32)


def position():
    xh, core = lax.axis_index("xh"), lax.axis_index("core")
    return 2 * xh + core, core, xh


def first_kernel(
    q_hbm, k_hbm, v_hbm, decay_hbm, write_hbm, cov_hbm, val_hbm,
    msg, cov, val, q32, k32, v_mine, total_out, mix_out,
    q_in, k_in, v_in, decay_in, write_in, z32, small_sem, big_sem, val_sem,
):
    start = pl.multiple_of(position()[0] * PART, PART)
    ends = [
        (decay_hbm, decay_in),
        (write_hbm, write_in),
        (q_hbm, q_in),
        (k_hbm, k_in),
        (v_hbm.at[:, :, pl.ds(start, PART)], v_in),
    ]
    small = [pltpu.make_async_copy(a, b, small_sem.at[n]) for n, (a, b) in enumerate(ends)]
    big = [
        [
            pltpu.make_async_copy(
                cov_hbm.at[pl.ds(2 * p, 2), :, pl.ds(PART * b, PART)],
                cov.at[pl.ds(2 * p, 2), b],
                big_sem.at[p, b],
            )
            for b in range(BLOCKS)
        ]
        for p in range(SEQS // 2)
    ]
    big.append([pltpu.make_async_copy(val_hbm, val, val_sem)])
    for c in small + big[0] + big[1] + big[2] + big[3]:
        c.start()
    for c in small[:2]:
        c.wait()
    total, mix = coefficients(decay_in[...], write_in[...])
    total_out[...] = jnp.broadcast_to(total, total_out.shape)
    mix_out[...] = mix
    for c, x, out in zip(small[2:], (q_in, k_in, v_in), (q32, k32, v_mine)):
        c.wait()
        stack(x, out)
    keys = k32[...].astype(BF16)
    keys_mine = k32[:, pl.ds(start, PART)].astype(BF16)
    dots = mm(q32[...].astype(BF16), keys, NT)
    base = mm_wide(mix * dots, keys_mine)
    first = lax.broadcasted_iota(jnp.int32, (8, 1), 0) < DRAFT

    def by_columns(p, pieces):
        both = jnp.concatenate(pieces, axis=0)
        res = [jnp.concatenate([mm(both, cov[2 * p + n, b]) for b in range(BLOCKS)], axis=1) for n in range(2)]
        z = jnp.where(first, res[0][:8] + res[0][8:], res[1][:8] + res[1][8:])
        z32[8 * p : 8 * p + 8, :] = z * total[8 * p : 8 * p + 8]

    held = None
    for p in range(SEQS // 2):
        for c in big[p]:
            c.wait()
        if p == 0:
            for c in big[4]:
                c.start()
        slab = q32[8 * p : 8 * p + 8, :].astype(BF16)
        res = [by_rows(slab, cov, 2 * p + n) for n in range(2)]
        y = jnp.where(first, res[0], res[1]) * total[8 * p : 8 * p + 8] + base[8 * p : 8 * p + 8]
        pieces = halves(y)
        msg[8 * p : 8 * p + 8, DK : DK + PART] = pieces[0]
        msg[8 * p : 8 * p + 8, DK + PART :] = pieces[1]
        if held is not None:
            by_columns(*held)
        held = (p, pieces)
    y_hi, y_lo = msg[:, DK : DK + PART], msg[:, DK + PART :]
    dots = mm(y_hi, keys_mine, NT) + mm(y_lo, keys_mine, NT)
    low_rank = mm_wide(mix * dots, keys)
    by_columns(*held)
    msg[:, :DK] = (z32[...] + low_rank).astype(BF16)
    big[4][0].wait()


def second_kernel(
    ridge, gathered, cov, val, q32, k32, v_mine, total_in, mix_in, sent, lhs, low, share_out,
    y32, w32, d32, x32, aw32,
):
    total, shift, mix = total_in[:, :1], ridge[0:1, 0:1], mix_in[...]
    me, core, _ = position()
    mine = pl.ds(pl.multiple_of(me * PART, PART), PART)
    first = lax.broadcasted_iota(jnp.int32, (8, 1), 0) < DRAFT

    def dot(a, b):
        return jnp.sum(a * b, axis=1, keepdims=True)

    for g in range(4):
        y32[:, g * PART : (g + 1) * PART] = gathered[g, :, DK : DK + PART].astype(F32) + gathered[
            g, :, DK + PART :
        ].astype(F32)
    w = y32[...]
    y32[...] = w + shift * q32[...]
    w = shift * (w + y32[...])
    for g in range(4):
        w = w + gathered[g, :, :DK].astype(F32)
    w32[...] = w
    keys = k32[...].astype(BF16)
    keys_mine = k32[:, mine].astype(BF16)
    for p in range(SEQS // 2):
        rows = slice(8 * p, 8 * p + 8)
        pieces = jnp.concatenate(halves(w32[rows, :]), axis=0)
        res = [by_rows(pieces, cov, 2 * p + n) for n in range(2)]
        aw32[rows, :] = jnp.where(first, res[0][:8] + res[0][8:], res[1][:8] + res[1][8:]) * total[rows]
    dots_w = mm(jnp.concatenate(halves(w32[...]), axis=0), keys, NT)
    image_w = aw32[...] + mm_wide(mix * (dots_w[:ROWS] + dots_w[ROWS:]), keys_mine) + shift * w32[:, mine]

    q, y, w = q32[...], y32[...], w32[...]
    rr0 = dot(q, q)
    a0 = rr0 / dot(q, y)
    res1 = q - a0 * y
    rr1 = dot(res1, res1)
    b0 = rr1 / rr0
    dir1 = res1 + b0 * q
    image1 = (1.0 + b0) * y - a0 * w
    a1 = rr1 / dot(dir1, image1)
    sol2 = a0 * q + a1 * dir1
    res2 = res1 - a1 * image1
    rr2 = dot(res2, res2)
    b1 = rr2 / rr1
    dir2 = res2 + b1 * dir1
    d32[...] = dir2
    x32[...] = sol2
    y, w = y32[:, mine], w32[:, mine]
    image2 = y - a0 * w - a1 * ((1.0 + b0) * w - a0 * image_w) + b1 * ((1.0 + b0) * y - a0 * w)
    share = jnp.broadcast_to(dot(d32[:, mine], image2) / rr2, (ROWS, 128))
    sent[:, 4 * PART :] = share.astype(BF16)
    share_out[...] = share
    for p in range(SEQS // 2):
        rows = slice(8 * p, 8 * p + 8)
        both = [x32[rows, mine].astype(BF16), d32[rows, mine].astype(BF16)]
        lhs[2 * 8 * p : 2 * 8 * (p + 1), :] = jnp.concatenate(both, axis=0)
        if p == 2:
            dots = mm(jnp.concatenate(halves(x32[...]) + (d32[...].astype(BF16),), axis=0), keys, NT)
        by_values(lhs, val, total, 1 - core, p, sent)
    values = v_mine[...].astype(BF16)
    low[:, :PART] = mm_wide(mix * (dots[:ROWS] + dots[ROWS : 2 * ROWS]), values)
    low[:, PART:] = mm_wide(mix * dots[2 * ROWS :], values)


def by_values(lhs, val, total, core, p, out):
    rows = slice(8 * p, 8 * p + 8)
    first = lax.broadcasted_iota(jnp.int32, (8, 1), 0) < DRAFT
    both = lhs[16 * p : 16 * p + 16, :]
    for x in range(2):
        entries = pl.ds(pl.multiple_of((2 * x + core) * PART, PART), PART)
        res = [mm(both, val[2 * p + n, entries, :], NT) for n in range(2)]
        for m in range(2):
            half = slice(8 * m, 8 * m + 8)
            part = jnp.where(first, res[0][half], res[1][half]) * total[rows]
            out[rows, (2 * m + x) * PART : (2 * m + x + 1) * PART] = part.astype(out.dtype)


def own_kernel(val, lhs, total_in, low, share, kept):
    _, core, xh = position()
    total = total_in[:, :1]
    for p in range(SEQS // 2):
        by_values(lhs, val, total, core, p, kept)
    kept[:, 4 * PART :] = share[...]
    for m in range(2):
        kept[:, pl.ds(pl.multiple_of((2 * m + xh) * PART, PART), PART)] += low[:, m * PART : (m + 1) * PART]


def project(scaled, weight, core, out):
    step = 512
    for x in range(2):
        for n in range(2048 // step):
            cols = pl.ds(pl.multiple_of((2 * x + core) * 2048 + n * step, step), step)
            part = mm(scaled, weight[:, cols])
            for m in range(step // 128):
                out[16 * x + n * (step // 128) + m] = part[:, 128 * m : 128 * (m + 1)].astype(out.dtype)


def third_kernel(mine, arrived, gain, weight, sent, scaled, squares):
    _, core, xh = position()
    total = mine[...].astype(F32) + arrived[...].astype(F32)
    a2 = 1.0 / total[:, 4 * PART : 4 * PART + 1]
    readout = total[:, : 2 * PART] + a2 * total[:, 2 * PART : 4 * PART]
    own = jnp.where(xh == 0, readout[:, :PART], readout[:, PART:])
    scaled[...] = (own * gain[...]).astype(BF16)
    project(scaled[...], weight, 1 - core, sent)
    squares[...] = jnp.broadcast_to(jnp.sum(readout * readout, axis=1, keepdims=True), (ROWS, 128))
    sent[32], sent[33] = halves(squares[...])


def last_kernel(scaled, weight, kept):
    project(scaled[...], weight, position()[1], kept)


def swapped(x, axis):
    return lax.ppermute(x, axis, [(0, 1), (1, 0)])


def params(mib):
    return pltpu.CompilerParams(vmem_limit_bytes=mib << 20)


def body(
    new_queries, new_keys, new_values, decay_gate, write_gate,
    ridge_shift, norm_gain, cov_state, value_state, out_weight,
):
    q, k, v = (x[:, 0] for x in (new_queries, new_keys, new_values))
    decay, write = (x[:, 0].T for x in (decay_gate, write_gate))
    cov, val, weight = cov_state[:, 0], value_state[:, 0], out_weight[0]

    estimate = pl.CostEstimate(flops=1 << 28, bytes_accessed=1 << 21, transcendentals=0)
    in_hbm = [
        pltpu.with_memory_space_constraint(x, pltpu.HBM)
        for x in (q, k, v, decay, write, cov, val)
    ]
    msg, *carried = pl.pallas_call(
        first_kernel,
        name="first",
        out_shape=(
            pltpu.VMEM((ROWS, DK + 2 * PART), BF16),
            pltpu.VMEM((SEQS, BLOCKS, PART, PART), BF16),
            pltpu.VMEM((SEQS, DV, PART), BF16),
            pltpu.VMEM((ROWS, DK), F32),
            pltpu.VMEM((ROWS, DK), F32),
            pltpu.VMEM((ROWS, PART), F32),
            pltpu.VMEM((ROWS, 128), F32),
            pltpu.VMEM((ROWS, ROWS), F32),
        ),
        in_specs=[HBM] * 7,
        out_specs=(VMEM,) * 8,
        scratch_shapes=[
            pltpu.VMEM((SEQS, DRAFT, DK), BF16),
            pltpu.VMEM((SEQS, DRAFT, DK), BF16),
            pltpu.VMEM((SEQS, DRAFT, PART), BF16),
            pltpu.VMEM((DRAFT, SEQS), F32),
            pltpu.VMEM((DRAFT, SEQS), F32),
            pltpu.VMEM((ROWS, DK), F32),
            pltpu.SemaphoreType.DMA((5,)),
            pltpu.SemaphoreType.DMA((SEQS // 2, BLOCKS)),
            pltpu.SemaphoreType.DMA,
        ],
        compiler_params=params(16),
    )(*in_hbm)
    gathered = lax.all_gather(msg, KEY)
    sent, lhs, low, share = pl.pallas_call(
        second_kernel,
        name="second",
        out_shape=(
            pltpu.VMEM((ROWS, 4 * PART + 128), BF16),
            pltpu.VMEM((2 * ROWS, PART), BF16),
            pltpu.VMEM((ROWS, 2 * PART), F32),
            pltpu.VMEM((ROWS, 128), F32),
        ),
        in_specs=[VMEM] * 9,
        out_specs=(VMEM,) * 4,
        scratch_shapes=[pltpu.VMEM((ROWS, n), F32) for n in (DK, DK, DK, DK, PART)],
        compiler_params=params(16),
    )(jnp.broadcast_to(ridge_shift[None], (8, 128)), gathered, *carried)
    kept = pl.pallas_call(
        own_kernel,
        name="own",
        out_shape=pltpu.VMEM((ROWS, 4 * PART + 128), F32),
        in_specs=[VMEM] * 5,
        out_specs=VMEM,
        compiler_params=params(16),
        cost_estimate=estimate,
    )(carried[1], lhs, carried[5], low, share)
    pair = (kept + swapped(sent, "core").astype(F32)).astype(BF16)
    other = swapped(pair, "xh")
    sent, scaled, squares = pl.pallas_call(
        third_kernel,
        name="third",
        out_shape=(
            pltpu.VMEM((34, ROWS, 128), BF16),
            pltpu.VMEM((ROWS, PART), BF16),
            pltpu.VMEM((ROWS, 128), F32),
        ),
        in_specs=[VMEM] * 4,
        out_specs=(VMEM,) * 3,
        compiler_params=params(16),
    )(pair, other, norm_gain, weight)
    kept = pl.pallas_call(
        last_kernel,
        name="last",
        out_shape=pltpu.VMEM((32, ROWS, 128), F32),
        in_specs=[VMEM] * 2,
        out_specs=VMEM,
        compiler_params=params(16),
        cost_estimate=estimate,
    )(scaled, weight)
    arrived = swapped(sent, "core").astype(F32)
    scale = lax.rsqrt((squares + arrived[32] + arrived[33]) * (1.0 / DV) + 1e-06)
    part = ((kept + arrived[:32]) * scale).astype(BF16)
    landed = lax.all_to_all(part, ("xh", "head"), 0, 0, tiled=True)
    out = landed.astype(F32).sum(axis=0).astype(BF16)
    return out.reshape(SEQS, DRAFT, 128)


def solution(mesh):
    fine = Mesh(mesh.devices.reshape(2, 2, *mesh.devices.shape[1:]), ("xh", "core", "head", "batch"))
    placed = (
        P("batch", "head", None, None),
        P("batch", "head", None, None),
        P("batch", "head", None, None),
        P("batch", "head", None),
        P("batch", "head", None),
        P("head"),
        P("head", KEY),
        P("batch", "head", KEY, None),
        P("batch", "head", None, KEY),
        P("head", KEY, None),
    )
    return jax.shard_map(
        body,
        mesh=fine,
        in_specs=placed,
        out_specs=P("batch", None, ("xh", "core", "head")),
        check_vma=False,
    )
```

```python
import jax
import jax.numpy as jnp
from jax import lax
from jax.experimental import pallas as pl
from jax.experimental.pallas import tpu as pltpu
from jax.sharding import Mesh, PartitionSpec as P

DRAFT = 4
SEQS = 8
ROWS = SEQS * DRAFT
DK = 1024
DV = 1024
PART = 256
BLOCKS = DK // PART
SLOT = 2 * PART
SHARE = 2 * SLOT
F32 = jnp.float32
BF16 = jnp.bfloat16
KEY = ("xh", "core")
HBM = pl.BlockSpec(memory_space=pltpu.HBM)
VMEM = pl.BlockSpec(memory_space=pltpu.VMEM)
NT = (((1,), (1,)), ((), ()))
NN = (((1,), (0,)), ((), ()))


def mm(a, b, dims=NN):
    return lax.dot_general(a, b, dims, preferred_element_type=F32)


def halves(x):
    hi = x.astype(BF16)
    return hi, (x - hi.astype(F32)).astype(BF16)


def mm_wide(a, b):
    hi, lo = halves(a)
    return mm(hi, b) + mm(lo, b)


def by_rows(a, cov, s):
    return sum(mm(a[:, PART * b : PART * (b + 1)], cov[s, b], NT) for b in range(BLOCKS))


def coefficients(decay, write):
    totals = [decay[0:1]]
    for t in range(1, DRAFT):
        totals.append(totals[-1] * decay[t : t + 1])
    row = lax.broadcasted_iota(jnp.int32, (ROWS, SEQS), 0)
    seq = lax.broadcasted_iota(jnp.int32, (ROWS, SEQS), 1)
    token = row % DRAFT

    def column(rows):
        spread = jnp.zeros((ROWS, SEQS), F32)
        for t in range(DRAFT):
            spread = jnp.where(token == t, jnp.broadcast_to(rows[t], (ROWS, SEQS)), spread)
        return jnp.sum(jnp.where(row // DRAFT == seq, spread, 0.0), axis=1, keepdims=True)

    total = column(totals)
    written = column([write[t : t + 1] for t in range(DRAFT)])
    i = lax.broadcasted_iota(jnp.int32, (ROWS, ROWS), 0)
    j = lax.broadcasted_iota(jnp.int32, (ROWS, ROWS), 1)

    def as_row(col):
        return jnp.sum(jnp.where(i == j, jnp.broadcast_to(col, (ROWS, ROWS)), 0.0), axis=0, keepdims=True)

    kept = (i // DRAFT == j // DRAFT) & (j <= i)
    mix = jnp.where(kept, as_row(written) * (total / as_row(total)), 0.0)
    return total, mix


def stack(ref, out):
    for s in range(SEQS):
        out[DRAFT * s : DRAFT * (s + 1), :] = ref[s].astype(F32)


def position():
    xh, core = lax.axis_index("xh"), lax.axis_index("core")
    return 2 * xh + core, core, xh


def first_kernel(
    q_hbm, k_hbm, v_hbm, decay_hbm, write_hbm, cov_hbm, val_hbm,
    msg, cov, val, q32, k32, values, total_out, mix_out,
    q_in, k_in, v_in, v_across, decay_in, write_in, small_sem, big_sem, val_sem,
):
    me, core, xh = position()
    start = pl.multiple_of(me * PART, PART)
    across = pl.multiple_of((2 * (1 - xh) + core) * PART, PART)
    ends = [
        (decay_hbm, decay_in),
        (write_hbm, write_in),
        (q_hbm, q_in),
        (k_hbm, k_in),
        (v_hbm.at[:, :, pl.ds(start, PART)], v_in),
        (v_hbm.at[:, :, pl.ds(across, PART)], v_across),
    ]
    small = [pltpu.make_async_copy(a, b, small_sem.at[n]) for n, (a, b) in enumerate(ends)]
    big = [
        [
            pltpu.make_async_copy(
                cov_hbm.at[pl.ds(2 * p, 2), :, pl.ds(PART * b, PART)],
                cov.at[pl.ds(2 * p, 2), b],
                big_sem.at[p, b],
            )
            for b in range(BLOCKS)
        ]
        for p in range(SEQS // 2)
    ]
    big.append([pltpu.make_async_copy(val_hbm, val, val_sem)])
    for c in small + big[0] + big[1] + big[2] + big[3]:
        c.start()
    for c in small[:2]:
        c.wait()
    total, mix = coefficients(decay_in[...], write_in[...])
    total_out[...] = jnp.broadcast_to(total, total_out.shape)
    mix_out[...] = mix
    out_of = (q32, k32, values.at[:, :PART], values.at[:, PART:])
    for c, x, out in zip(small[2:], (q_in, k_in, v_in, v_across), out_of):
        c.wait()
        stack(x, out)
    keys = k32[...].astype(BF16)
    keys_mine = k32[:, pl.ds(start, PART)].astype(BF16)
    dots = mm(q32[...].astype(BF16), keys, NT)
    base = mm_wide(mix * dots, keys_mine)
    first = lax.broadcasted_iota(jnp.int32, (8, 1), 0) < DRAFT

    def by_columns(p, pieces):
        both = jnp.concatenate(pieces, axis=0)
        res = [jnp.concatenate([mm(both, cov[2 * p + n, b]) for b in range(BLOCKS)], axis=1) for n in range(2)]
        z = jnp.where(first, res[0][:8] + res[0][8:], res[1][:8] + res[1][8:])
        msg[8 * p : 8 * p + 8, :DK] = (z * total[8 * p : 8 * p + 8]).astype(BF16)

    held = None
    for p in range(SEQS // 2):
        for c in big[p]:
            c.wait()
        if p == 0:
            for c in big[4]:
                c.start()
        slab = q32[8 * p : 8 * p + 8, :].astype(BF16)
        res = [by_rows(slab, cov, 2 * p + n) for n in range(2)]
        y = jnp.where(first, res[0], res[1]) * total[8 * p : 8 * p + 8] + base[8 * p : 8 * p + 8]
        pieces = halves(y)
        msg[8 * p : 8 * p + 8, DK : DK + PART] = pieces[0]
        msg[8 * p : 8 * p + 8, DK + PART :] = pieces[1]
        if held is not None:
            by_columns(*held)
        held = (p, pieces)
    by_columns(*held)
    big[4][0].wait()


def second_kernel(
    ridge, gathered, cov, val, q32, k32, values_in, total_in, mix_in, sent, lhs, low, share_out,
    p32, y32, w32, low32, d32, x32, ap32, aw32, dm32,
):
    total, shift, mix = total_in[:, :1], ridge[0:1, 0:1], mix_in[...]
    me, core, xh = position()
    mine = pl.ds(pl.multiple_of(me * PART, PART), PART)
    first = lax.broadcasted_iota(jnp.int32, (8, 1), 0) < DRAFT

    def dot(a, b):
        return jnp.sum(a * b, axis=1, keepdims=True)

    def dots_of(a, b):
        res = mm(jnp.concatenate(halves(a), axis=0), b, NT)
        return res[:ROWS] + res[ROWS:]

    for g in range(BLOCKS):
        p32[:, g * PART : (g + 1) * PART] = gathered[g, :, DK : DK + PART].astype(F32) + gathered[
            g, :, DK + PART :
        ].astype(F32)
    keys = k32[...].astype(BF16)
    keys_mine = k32[:, mine].astype(BF16)
    low32[...] = mm_wide(mix * dots_of(p32[...], keys), keys)
    p = p32[...]
    y = p + shift * q32[...]
    y32[...] = y
    w = shift * (p + y)
    for g in range(BLOCKS):
        w = w + gathered[g, :, :DK].astype(F32)
    w32[...] = w + low32[...]
    for p in range(SEQS // 2):
        rows = slice(8 * p, 8 * p + 8)
        pieces = jnp.concatenate(halves(p32[rows, :]) + halves(w32[rows, :]), axis=0)
        res = [by_rows(pieces, cov, 2 * p + n) for n in range(2)]
        res = [(r[:8] + r[8:16], r[16:24] + r[24:]) for r in res]
        ap32[rows, :] = jnp.where(first, res[0][0], res[1][0]) * total[rows]
        aw32[rows, :] = jnp.where(first, res[0][1], res[1][1]) * total[rows]
    image_w = aw32[...] + mm_wide(mix * dots_of(w32[...], keys), keys_mine) + shift * w32[:, mine]

    q, y, w = q32[...], y32[...], w32[...]
    rr0 = dot(q, q)
    a0 = rr0 / dot(q, y)
    res1 = q - a0 * y
    rr1 = dot(res1, res1)
    b0 = rr1 / rr0
    dir1 = res1 + b0 * q
    image1 = (1.0 + b0) * y - a0 * w
    a1 = rr1 / dot(dir1, image1)
    sol2 = a0 * q + a1 * dir1
    res2 = res1 - a1 * image1
    rr2 = dot(res2, res2)
    b1 = rr2 / rr1
    d32[...] = res2 + b1 * dir1
    x32[...] = sol2
    q, y, p = q32[:, mine], y32[:, mine], p32[:, mine]
    w = ap32[...] + low32[:, mine] + shift * (p + y)
    res1 = q - a0 * y
    dir1 = res1 + b0 * q
    image1 = (1.0 + b0) * y - a0 * w
    dir2 = res1 - a1 * image1 + b1 * dir1
    dm32[...] = dir2
    image2 = y - a0 * w - a1 * ((1.0 + b0) * w - a0 * image_w) + b1 * image1
    known = d32[:, mine]
    share = jnp.broadcast_to(dot(known, image2) / rr2, (ROWS, 64))
    missed = mix * mm((dir2 - known).astype(BF16), keys_mine, NT)
    share = jnp.concatenate([share, missed, jnp.zeros((ROWS, 32), F32)], axis=1)
    share_out[...] = share
    for p in range(SEQS // 2):
        rows = slice(8 * p, 8 * p + 8)
        both = [x32[rows, mine].astype(BF16), dm32[rows, :].astype(BF16)]
        lhs[2 * 8 * p : 2 * 8 * (p + 1), :] = jnp.concatenate(both, axis=0)
        if p == 2:
            dots = mm(jnp.concatenate(halves(x32[...]) + (d32[...].astype(BF16),), axis=0), keys, NT)
        by_values(lhs, val, total, xh, 1 - core, p, sent)
    sent[:, SHARE:] = share.astype(BF16)
    values = values_in[:, :PART].astype(BF16)
    low[:, :PART] = mm_wide(mix * (dots[:ROWS] + dots[ROWS : 2 * ROWS]), values)
    low[:, PART:] = mm_wide(mix * dots[2 * ROWS :], values)


def by_values(lhs, val, total, xh, core, p, out):
    rows = slice(8 * p, 8 * p + 8)
    first = lax.broadcasted_iota(jnp.int32, (8, 1), 0) < DRAFT
    both = lhs[16 * p : 16 * p + 16, :]
    for slot, x in enumerate((xh, 1 - xh)):
        entries = pl.ds(pl.multiple_of((2 * x + core) * PART, PART), PART)
        res = [mm(both, val[2 * p + n, entries, :], NT) for n in range(2)]
        for m in range(2):
            half = slice(8 * m, 8 * m + 8)
            part = jnp.where(first, res[0][half], res[1][half]) * total[rows]
            at = slot * SLOT + m * PART
            out[rows, at : at + PART] = part.astype(out.dtype)


def own_kernel(val, lhs, total_in, low, share, kept):
    _, core, xh = position()
    total = total_in[:, :1]
    for p in range(SEQS // 2):
        by_values(lhs, val, total, xh, core, p, kept)
    kept[:, SHARE:] = share[...]
    kept[:, : 2 * PART] += low[...]


def project(scaled, weight, core, out):
    step = 512
    for x in range(2):
        for n in range(2048 // step):
            cols = pl.ds(pl.multiple_of((2 * x + core) * 2048 + n * step, step), step)
            part = mm(scaled, weight[:, cols])
            for m in range(step // 128):
                out[16 * x + n * (step // 128) + m] = part[:, 128 * m : 128 * (m + 1)].astype(out.dtype)


def third_kernel(mine, partner, arrived, values, gain, weight, sent, scaled, squares):
    pair = mine[...] + partner[...].astype(F32)
    other = arrived[...].astype(F32)
    total = [pair[:, SLOT * n : SLOT * (n + 1)] + other[:, SLOT * (1 - n) : SLOT * (2 - n)] for n in range(2)]
    share = pair[:, SHARE:] + other[:, SHARE:]
    a2 = 1.0 / share[:, :1]
    missed = mm(share[:, 64:96].astype(BF16), values[...].astype(BF16))
    readout = [
        total[n][:, :PART] + a2 * (total[n][:, PART:] + missed[:, PART * n : PART * (n + 1)]) for n in range(2)
    ]
    scaled[...] = (readout[0] * gain[...]).astype(BF16)
    project(scaled[...], weight, 1 - position()[1], sent)
    both = readout[0] * readout[0] + readout[1] * readout[1]
    squares[...] = jnp.broadcast_to(jnp.sum(both, axis=1, keepdims=True), (ROWS, 128))
    sent[32], sent[33] = halves(squares[...])


def last_kernel(scaled, weight, kept):
    project(scaled[...], weight, position()[1], kept)


def join_kernel(kept, arrived, squares, out):
    sums = squares[...] + arrived[32].astype(F32) + arrived[33].astype(F32)
    scale = lax.rsqrt(sums * (1.0 / DV) + 1e-06)
    for n in range(32):
        out[n] = ((kept[n] + arrived[n].astype(F32)) * scale).astype(BF16)


def swapped(x, axis):
    return lax.ppermute(x, axis, [(0, 1), (1, 0)])


def params(mib):
    return pltpu.CompilerParams(vmem_limit_bytes=mib << 20)


def body(
    new_queries, new_keys, new_values, decay_gate, write_gate,
    ridge_shift, norm_gain, cov_state, value_state, out_weight,
):
    q, k, v = (x[:, 0] for x in (new_queries, new_keys, new_values))
    decay, write = (x[:, 0].T for x in (decay_gate, write_gate))
    cov, val, weight = cov_state[:, 0], value_state[:, 0], out_weight[0]

    estimate = pl.CostEstimate(flops=1 << 28, bytes_accessed=1 << 21, transcendentals=0)
    in_hbm = [
        pltpu.with_memory_space_constraint(x, pltpu.HBM)
        for x in (q, k, v, decay, write, cov, val)
    ]
    msg, *carried = pl.pallas_call(
        first_kernel,
        name="first",
        out_shape=(
            pltpu.VMEM((ROWS, DK + 2 * PART), BF16),
            pltpu.VMEM((SEQS, BLOCKS, PART, PART), BF16),
            pltpu.VMEM((SEQS, DV, PART), BF16),
            pltpu.VMEM((ROWS, DK), F32),
            pltpu.VMEM((ROWS, DK), F32),
            pltpu.VMEM((ROWS, SLOT), F32),
            pltpu.VMEM((ROWS, 128), F32),
            pltpu.VMEM((ROWS, ROWS), F32),
        ),
        in_specs=[HBM] * 7,
        out_specs=(VMEM,) * 8,
        scratch_shapes=[
            pltpu.VMEM((SEQS, DRAFT, DK), BF16),
            pltpu.VMEM((SEQS, DRAFT, DK), BF16),
            pltpu.VMEM((SEQS, DRAFT, PART), BF16),
            pltpu.VMEM((SEQS, DRAFT, PART), BF16),
            pltpu.VMEM((DRAFT, SEQS), F32),
            pltpu.VMEM((DRAFT, SEQS), F32),
            pltpu.SemaphoreType.DMA((6,)),
            pltpu.SemaphoreType.DMA((SEQS // 2, BLOCKS)),
            pltpu.SemaphoreType.DMA,
        ],
        compiler_params=params(16),
    )(*in_hbm)
    gathered = lax.all_gather(msg, KEY)
    sent, lhs, low, share = pl.pallas_call(
        second_kernel,
        name="second",
        out_shape=(
            pltpu.VMEM((ROWS, SHARE + 128), BF16),
            pltpu.VMEM((2 * ROWS, PART), BF16),
            pltpu.VMEM((ROWS, 2 * PART), F32),
            pltpu.VMEM((ROWS, 128), F32),
        ),
        in_specs=[VMEM] * 9,
        out_specs=(VMEM,) * 4,
        scratch_shapes=[pltpu.VMEM((ROWS, n), F32) for n in [DK] * 6 + [PART] * 3],
        compiler_params=params(16),
    )(jnp.broadcast_to(ridge_shift[None], (8, 128)), gathered, *carried)
    kept = pl.pallas_call(
        own_kernel,
        name="own",
        out_shape=pltpu.VMEM((ROWS, SHARE + 128), F32),
        in_specs=[VMEM] * 5,
        out_specs=VMEM,
        compiler_params=params(16),
        cost_estimate=estimate,
    )(carried[1], lhs, carried[5], low, share)
    partner = swapped(sent, "core")
    other = swapped((kept + partner.astype(F32)).astype(BF16), "xh")
    sent, scaled, squares = pl.pallas_call(
        third_kernel,
        name="third",
        out_shape=(
            pltpu.VMEM((34, ROWS, 128), BF16),
            pltpu.VMEM((ROWS, PART), BF16),
            pltpu.VMEM((ROWS, 128), F32),
        ),
        in_specs=[VMEM] * 6,
        out_specs=(VMEM,) * 3,
        compiler_params=params(16),
    )(kept, partner, other, carried[4], norm_gain, weight)
    part = pl.pallas_call(
        last_kernel,
        name="last",
        out_shape=pltpu.VMEM((32, ROWS, 128), F32),
        in_specs=[VMEM] * 2,
        out_specs=VMEM,
        compiler_params=params(16),
        cost_estimate=estimate,
    )(scaled, weight)
    part = pl.pallas_call(
        join_kernel,
        name="join",
        out_shape=pltpu.VMEM((32, ROWS, 128), BF16),
        in_specs=[VMEM] * 3,
        out_specs=VMEM,
        compiler_params=params(16),
    )(part, swapped(sent, "core"), squares)
    landed = lax.all_to_all(part, ("xh", "head"), 0, 0, tiled=True)
    return landed.astype(F32).sum(axis=0).astype(BF16).reshape(SEQS, DRAFT, 128)


def solution(mesh):
    fine = Mesh(mesh.devices.reshape(2, 2, *mesh.devices.shape[1:]), ("xh", "core", "head", "batch"))
    placed = (
        P("batch", "head", None, None),
        P("batch", "head", None, None),
        P("batch", "head", None, None),
        P("batch", "head", None),
        P("batch", "head", None),
        P("head"),
        P("head", KEY),
        P("batch", "head", KEY, None),
        P("batch", "head", None, KEY),
        P("head", KEY, None),
    )
    return jax.shard_map(
        body,
        mesh=fine,
        in_specs=placed,
        out_specs=P("batch", None, ("xh", "core", "head")),
        check_vma=False,
    )
```

```python
import jax
import jax.numpy as jnp
from jax import lax
from jax.experimental import pallas as pl
from jax.experimental.pallas import tpu as pltpu
from jax.sharding import Mesh, PartitionSpec as P

DRAFT = 4
SEQS = 8
ROWS = SEQS * DRAFT
DK = 1024
DV = 1024
PART = 256
BLOCKS = DK // PART
SLOT = 2 * PART
SHARE = 2 * SLOT
F32 = jnp.float32
BF16 = jnp.bfloat16
KEY = ("xh", "core")
HBM = pl.BlockSpec(memory_space=pltpu.HBM)
VMEM = pl.BlockSpec(memory_space=pltpu.VMEM)
NT = (((1,), (1,)), ((), ()))
NN = (((1,), (0,)), ((), ()))


def mm(a, b, dims=NN):
    return lax.dot_general(a, b, dims, preferred_element_type=F32)


def halves(x):
    hi = x.astype(BF16)
    return hi, (x - hi.astype(F32)).astype(BF16)


def mm_wide(a, b):
    hi, lo = halves(a)
    return mm(hi, b) + mm(lo, b)


def by_rows(a, cov, s):
    return sum(mm(a[:, PART * b : PART * (b + 1)], cov[s, b], NT) for b in range(BLOCKS))


def coefficients(decay, write):
    totals = [decay[0:1]]
    for t in range(1, DRAFT):
        totals.append(totals[-1] * decay[t : t + 1])
    row = lax.broadcasted_iota(jnp.int32, (ROWS, SEQS), 0)
    seq = lax.broadcasted_iota(jnp.int32, (ROWS, SEQS), 1)
    token = row % DRAFT

    def column(rows):
        spread = jnp.zeros((ROWS, SEQS), F32)
        for t in range(DRAFT):
            spread = jnp.where(token == t, jnp.broadcast_to(rows[t], (ROWS, SEQS)), spread)
        return jnp.sum(jnp.where(row // DRAFT == seq, spread, 0.0), axis=1, keepdims=True)

    total = column(totals)
    written = column([write[t : t + 1] for t in range(DRAFT)])
    i = lax.broadcasted_iota(jnp.int32, (ROWS, ROWS), 0)
    j = lax.broadcasted_iota(jnp.int32, (ROWS, ROWS), 1)

    def as_row(col):
        return jnp.sum(jnp.where(i == j, jnp.broadcast_to(col, (ROWS, ROWS)), 0.0), axis=0, keepdims=True)

    kept = (i // DRAFT == j // DRAFT) & (j <= i)
    mix = jnp.where(kept, as_row(written) * (total / as_row(total)), 0.0)
    return total, mix


def stack(ref, out):
    for s in range(SEQS):
        out[DRAFT * s : DRAFT * (s + 1), :] = ref[s].astype(F32)


def position():
    xh, core = lax.axis_index("xh"), lax.axis_index("core")
    return 2 * xh + core, core, xh


def first_kernel(
    q_hbm, k_hbm, v_hbm, decay_hbm, write_hbm, cov_hbm, val_hbm,
    msg, cov, val, q32, k32, values, total_out, mix_out, ck, cq,
    q_in, k_in, v_in, v_across, decay_in, write_in, small_sem, big_sem, val_sem,
):
    me, core, xh = position()
    start = pl.multiple_of(me * PART, PART)
    across = pl.multiple_of((2 * (1 - xh) + core) * PART, PART)
    ends = [
        (decay_hbm, decay_in),
        (write_hbm, write_in),
        (q_hbm, q_in),
        (k_hbm, k_in),
        (v_hbm.at[:, :, pl.ds(start, PART)], v_in),
        (v_hbm.at[:, :, pl.ds(across, PART)], v_across),
    ]
    small = [pltpu.make_async_copy(a, b, small_sem.at[n]) for n, (a, b) in enumerate(ends)]
    big = [
        [
            pltpu.make_async_copy(
                cov_hbm.at[pl.ds(2 * p, 2), :, pl.ds(PART * b, PART)],
                cov.at[pl.ds(2 * p, 2), b],
                big_sem.at[p, b],
            )
            for b in range(BLOCKS)
        ]
        for p in range(SEQS // 2)
    ]
    big.append([pltpu.make_async_copy(val_hbm, val, val_sem)])
    for c in small[:4] + big[0] + small[4:] + big[1] + big[2] + big[3] + big[4]:
        c.start()
    for c in small[:2]:
        c.wait()
    total, mix = coefficients(decay_in[...], write_in[...])
    total_out[...] = jnp.broadcast_to(total, total_out.shape)
    mix_out[...] = mix
    out_of = (q32, k32, values.at[:, :PART], values.at[:, PART:])
    for c, x, out in zip(small[2:], (q_in, k_in, v_in, v_across), out_of):
        c.wait()
        stack(x, out)
    keys = k32[...].astype(BF16)
    keys_mine = k32[:, pl.ds(start, PART)].astype(BF16)
    dots = mm(q32[...].astype(BF16), keys, NT)
    base = mm_wide(mix * dots, keys_mine)
    first = lax.broadcasted_iota(jnp.int32, (8, 1), 0) < DRAFT

    def by_columns(p, pieces):
        both = jnp.concatenate(pieces, axis=0)
        res = [jnp.concatenate([mm(both, cov[2 * p + n, b]) for b in range(BLOCKS)], axis=1) for n in range(2)]
        z = jnp.where(first, res[0][:8] + res[0][8:], res[1][:8] + res[1][8:])
        msg[8 * p : 8 * p + 8, :DK] = (z * total[8 * p : 8 * p + 8]).astype(BF16)

    held = None
    for p in range(SEQS // 2):
        for c in big[p]:
            c.wait()
        rows = slice(8 * p, 8 * p + 8)
        slab = jnp.concatenate([q32[rows, :].astype(BF16), k32[rows, :].astype(BF16)], axis=0)
        res = [by_rows(slab, cov, 2 * p + n) for n in range(2)]
        ck[rows, :] = jnp.where(first, res[0][8:], res[1][8:])
        part = jnp.where(first, res[0][:8], res[1][:8]) * total[rows]
        cq[rows, :] = part
        y = part + base[rows]
        pieces = halves(y)
        msg[8 * p : 8 * p + 8, DK : DK + PART] = pieces[0]
        msg[8 * p : 8 * p + 8, DK + PART :] = pieces[1]
        if held is not None:
            by_columns(*held)
        held = (p, pieces)
    by_columns(*held)
    big[4][0].wait()


def second_kernel(
    ridge, gathered, cov, val, q32, k32, values_in, total_in, mix_in, ck, cq, sent, lhs, low, share_out,
    p32, c32, y32, w32, low32, d32, x32, ap32, ac32, dm32,
):
    total, shift, mix = total_in[:, :1], ridge[0:1, 0:1], mix_in[...]
    me, core, xh = position()
    mine = pl.ds(pl.multiple_of(me * PART, PART), PART)
    first = lax.broadcasted_iota(jnp.int32, (8, 1), 0) < DRAFT

    def dot(a, b):
        return jnp.sum(a * b, axis=1, keepdims=True)

    def dots_of(a, b):
        res = mm(jnp.concatenate(halves(a), axis=0), b, NT)
        return res[:ROWS] + res[ROWS:]

    for g in range(BLOCKS):
        p32[:, g * PART : (g + 1) * PART] = gathered[g, :, DK : DK + PART].astype(F32) + gathered[
            g, :, DK + PART :
        ].astype(F32)
    keys = k32[...].astype(BF16)
    keys_mine = k32[:, mine].astype(BF16)
    c = gathered[0, :, :DK].astype(F32)
    for g in range(1, BLOCKS):
        c = c + gathered[g, :, :DK].astype(F32)
    c32[...] = c
    coef = mix * dots_of(p32[...], keys)
    for p in range(SEQS // 2):
        rows = slice(8 * p, 8 * p + 8)
        pieces = jnp.concatenate(halves(p32[rows, :]) + halves(c32[rows, :]), axis=0)
        res = [by_rows(pieces, cov, 2 * p + n) for n in range(2)]
        res = [(r[:8] + r[8:16], r[16:24] + r[24:]) for r in res]
        ap32[rows, :] = jnp.where(first, res[0][0], res[1][0]) * total[rows]
        ac32[rows, :] = jnp.where(first, res[0][1], res[1][1]) * total[rows]
        if p == 0:
            low32[...] = mm_wide(coef, keys)
            y32[...] = p32[...] + shift * q32[...]
            w32[...] = c32[...] + low32[...] + shift * (p32[...] + y32[...])
    ck_hi, ck_lo = halves(ck[...])
    state_w = ac32[...] + total * (mm_wide(coef, ck_hi) + mm(coef.astype(BF16), ck_lo))
    state_w = state_w + shift * (2.0 * ap32[...] + shift * cq[...])
    image_w = state_w + mm_wide(mix * dots_of(w32[...], keys), keys_mine) + shift * w32[:, mine]

    q, y, w = q32[...], y32[...], w32[...]
    rr0 = dot(q, q)
    a0 = rr0 / dot(q, y)
    res1 = q - a0 * y
    rr1 = dot(res1, res1)
    b0 = rr1 / rr0
    dir1 = res1 + b0 * q
    image1 = (1.0 + b0) * y - a0 * w
    a1 = rr1 / dot(dir1, image1)
    sol2 = a0 * q + a1 * dir1
    res2 = res1 - a1 * image1
    rr2 = dot(res2, res2)
    b1 = rr2 / rr1
    d32[...] = res2 + b1 * dir1
    x32[...] = sol2
    q, y, p = q32[:, mine], y32[:, mine], p32[:, mine]
    w = ap32[...] + low32[:, mine] + shift * (p + y)
    res1 = q - a0 * y
    dir1 = res1 + b0 * q
    image1 = (1.0 + b0) * y - a0 * w
    dir2 = res1 - a1 * image1 + b1 * dir1
    dm32[...] = dir2
    image2 = y - a0 * w - a1 * ((1.0 + b0) * w - a0 * image_w) + b1 * image1
    known = d32[:, mine]
    share = jnp.broadcast_to(dot(known, image2) / rr2, (ROWS, 64))
    missed = mix * mm((dir2 - known).astype(BF16), keys_mine, NT)
    share = jnp.concatenate([share, missed, jnp.zeros((ROWS, 32), F32)], axis=1)
    share_out[...] = share
    for p in range(SEQS // 2):
        rows = slice(8 * p, 8 * p + 8)
        both = [x32[rows, mine].astype(BF16), dm32[rows, :].astype(BF16)]
        lhs[2 * 8 * p : 2 * 8 * (p + 1), :] = jnp.concatenate(both, axis=0)
        if p == 2:
            dots = mm(jnp.concatenate(halves(x32[...]) + (d32[...].astype(BF16),), axis=0), keys, NT)
        by_values(lhs, val, total, xh, 1 - core, p, sent)
    sent[:, SHARE:] = share.astype(BF16)
    values = values_in[:, :PART].astype(BF16)
    low[:, :PART] = mm_wide(mix * (dots[:ROWS] + dots[ROWS : 2 * ROWS]), values)
    low[:, PART:] = mm_wide(mix * dots[2 * ROWS :], values)


def by_values(lhs, val, total, xh, core, p, out):
    rows = slice(8 * p, 8 * p + 8)
    first = lax.broadcasted_iota(jnp.int32, (8, 1), 0) < DRAFT
    both = lhs[16 * p : 16 * p + 16, :]
    for slot, x in enumerate((xh, 1 - xh)):
        entries = pl.ds(pl.multiple_of((2 * x + core) * PART, PART), PART)
        res = [mm(both, val[2 * p + n, entries, :], NT) for n in range(2)]
        for m in range(2):
            half = slice(8 * m, 8 * m + 8)
            part = jnp.where(first, res[0][half], res[1][half]) * total[rows]
            at = slot * SLOT + m * PART
            out[rows, at : at + PART] = part.astype(out.dtype)


def own_kernel(val, lhs, total_in, low, share, kept):
    _, core, xh = position()
    total = total_in[:, :1]
    for p in range(SEQS // 2):
        by_values(lhs, val, total, xh, core, p, kept)
    kept[:, SHARE:] = share[...]
    kept[:, : 2 * PART] += low[...]


def project(scaled, weight, core, out):
    step = 512
    for x in range(2):
        for n in range(2048 // step):
            cols = pl.ds(pl.multiple_of((2 * x + core) * 2048 + n * step, step), step)
            part = mm(scaled, weight[:, cols])
            for m in range(step // 128):
                out[16 * x + n * (step // 128) + m] = part[:, 128 * m : 128 * (m + 1)].astype(out.dtype)


def third_kernel(mine, partner, arrived, values, gain, weight, sent, scaled, squares):
    pair = mine[...] + partner[...].astype(F32)
    other = arrived[...].astype(F32)
    total = [pair[:, SLOT * n : SLOT * (n + 1)] + other[:, SLOT * (1 - n) : SLOT * (2 - n)] for n in range(2)]
    share = pair[:, SHARE:] + other[:, SHARE:]
    a2 = 1.0 / share[:, :1]
    missed = mm(share[:, 64:96].astype(BF16), values[...].astype(BF16))
    readout = [
        total[n][:, :PART] + a2 * (total[n][:, PART:] + missed[:, PART * n : PART * (n + 1)]) for n in range(2)
    ]
    scaled[...] = (readout[0] * gain[...]).astype(BF16)
    project(scaled[...], weight, 1 - position()[1], sent)
    both = readout[0] * readout[0] + readout[1] * readout[1]
    squares[...] = jnp.broadcast_to(jnp.sum(both, axis=1, keepdims=True), (ROWS, 128))
    sent[32], sent[33] = halves(squares[...])


def last_kernel(scaled, weight, kept):
    project(scaled[...], weight, position()[1], kept)


def join_kernel(kept, arrived, squares, out):
    sums = squares[...] + arrived[32].astype(F32) + arrived[33].astype(F32)
    scale = lax.rsqrt(sums * (1.0 / DV) + 1e-06)
    for n in range(32):
        out[n] = ((kept[n] + arrived[n].astype(F32)) * scale).astype(BF16)


def swapped(x, axis):
    return lax.ppermute(x, axis, [(0, 1), (1, 0)])


def params(mib):
    return pltpu.CompilerParams(vmem_limit_bytes=mib << 20)


def body(
    new_queries, new_keys, new_values, decay_gate, write_gate,
    ridge_shift, norm_gain, cov_state, value_state, out_weight,
):
    q, k, v = (x[:, 0] for x in (new_queries, new_keys, new_values))
    decay, write = (x[:, 0].T for x in (decay_gate, write_gate))
    cov, val, weight = cov_state[:, 0], value_state[:, 0], out_weight[0]

    estimate = pl.CostEstimate(flops=1 << 28, bytes_accessed=1 << 21, transcendentals=0)
    in_hbm = [
        pltpu.with_memory_space_constraint(x, pltpu.HBM)
        for x in (q, k, v, decay, write, cov, val)
    ]
    msg, *carried = pl.pallas_call(
        first_kernel,
        name="first",
        out_shape=(
            pltpu.VMEM((ROWS, DK + 2 * PART), BF16),
            pltpu.VMEM((SEQS, BLOCKS, PART, PART), BF16),
            pltpu.VMEM((SEQS, DV, PART), BF16),
            pltpu.VMEM((ROWS, DK), F32),
            pltpu.VMEM((ROWS, DK), F32),
            pltpu.VMEM((ROWS, SLOT), F32),
            pltpu.VMEM((ROWS, 128), F32),
            pltpu.VMEM((ROWS, ROWS), F32),
            pltpu.VMEM((ROWS, PART), F32),
            pltpu.VMEM((ROWS, PART), F32),
        ),
        in_specs=[HBM] * 7,
        out_specs=(VMEM,) * 10,
        scratch_shapes=[
            pltpu.VMEM((SEQS, DRAFT, DK), BF16),
            pltpu.VMEM((SEQS, DRAFT, DK), BF16),
            pltpu.VMEM((SEQS, DRAFT, PART), BF16),
            pltpu.VMEM((SEQS, DRAFT, PART), BF16),
            pltpu.VMEM((DRAFT, SEQS), F32),
            pltpu.VMEM((DRAFT, SEQS), F32),
            pltpu.SemaphoreType.DMA((6,)),
            pltpu.SemaphoreType.DMA((SEQS // 2, BLOCKS)),
            pltpu.SemaphoreType.DMA,
        ],
        compiler_params=params(16),
    )(*in_hbm)
    gathered = lax.all_gather(msg, KEY)
    sent, lhs, low, share = pl.pallas_call(
        second_kernel,
        name="second",
        out_shape=(
            pltpu.VMEM((ROWS, SHARE + 128), BF16),
            pltpu.VMEM((2 * ROWS, PART), BF16),
            pltpu.VMEM((ROWS, 2 * PART), F32),
            pltpu.VMEM((ROWS, 128), F32),
        ),
        in_specs=[VMEM] * 11,
        out_specs=(VMEM,) * 4,
        scratch_shapes=[pltpu.VMEM((ROWS, n), F32) for n in [DK] * 7 + [PART] * 3],
        compiler_params=params(16),
    )(jnp.broadcast_to(ridge_shift[None], (8, 128)), gathered, *carried)
    kept = pl.pallas_call(
        own_kernel,
        name="own",
        out_shape=pltpu.VMEM((ROWS, SHARE + 128), F32),
        in_specs=[VMEM] * 5,
        out_specs=VMEM,
        compiler_params=params(16),
        cost_estimate=estimate,
    )(carried[1], lhs, carried[5], low, share)
    partner = swapped(sent, "core")
    other = swapped((kept + partner.astype(F32)).astype(BF16), "xh")
    sent, scaled, squares = pl.pallas_call(
        third_kernel,
        name="third",
        out_shape=(
            pltpu.VMEM((34, ROWS, 128), BF16),
            pltpu.VMEM((ROWS, PART), BF16),
            pltpu.VMEM((ROWS, 128), F32),
        ),
        in_specs=[VMEM] * 6,
        out_specs=(VMEM,) * 3,
        compiler_params=params(16),
    )(kept, partner, other, carried[4], norm_gain, weight)
    part = pl.pallas_call(
        last_kernel,
        name="last",
        out_shape=pltpu.VMEM((32, ROWS, 128), F32),
        in_specs=[VMEM] * 2,
        out_specs=VMEM,
        compiler_params=params(16),
        cost_estimate=estimate,
    )(scaled, weight)
    part = pl.pallas_call(
        join_kernel,
        name="join",
        out_shape=pltpu.VMEM((32, ROWS, 128), BF16),
        in_specs=[VMEM] * 3,
        out_specs=VMEM,
        compiler_params=params(16),
    )(part, swapped(sent, "core"), squares)
    landed = lax.all_to_all(part, ("xh", "head"), 0, 0, tiled=True)
    return landed.astype(F32).sum(axis=0).astype(BF16).reshape(SEQS, DRAFT, 128)


def solution(mesh):
    fine = Mesh(mesh.devices.reshape(2, 2, *mesh.devices.shape[1:]), ("xh", "core", "head", "batch"))
    placed = (
        P("batch", "head", None, None),
        P("batch", "head", None, None),
        P("batch", "head", None, None),
        P("batch", "head", None),
        P("batch", "head", None),
        P("head"),
        P("head", KEY),
        P("batch", "head", KEY, None),
        P("batch", "head", None, KEY),
        P("head", KEY, None),
    )
    return jax.shard_map(
        body,
        mesh=fine,
        in_specs=placed,
        out_specs=P("batch", None, ("xh", "core", "head")),
        check_vma=False,
    )
```

```python
import jax
import jax.numpy as jnp
from jax import lax
from jax.experimental import pallas as pl
from jax.experimental.pallas import tpu as pltpu
from jax.sharding import Mesh, PartitionSpec as P

DRAFT = 4
SEQS = 8
ROWS = SEQS * DRAFT
DK = 1024
DV = 1024
PART = 256
BLOCKS = DK // PART
SLOT = 2 * PART
SHARE = 2 * SLOT
F32 = jnp.float32
BF16 = jnp.bfloat16
KEY = ("xh", "core")
HBM = pl.BlockSpec(memory_space=pltpu.HBM)
VMEM = pl.BlockSpec(memory_space=pltpu.VMEM)
NT = (((1,), (1,)), ((), ()))
NN = (((1,), (0,)), ((), ()))


def mm(a, b, dims=NN):
    return lax.dot_general(a, b, dims, preferred_element_type=F32)


def halves(x):
    hi = x.astype(BF16)
    return hi, (x - hi.astype(F32)).astype(BF16)


def mm_wide(a, b):
    hi, lo = halves(a)
    return mm(hi, b) + mm(lo, b)


def by_rows(a, cov, s):
    return sum(mm(a[:, PART * b : PART * (b + 1)], cov[s, b], NT) for b in range(BLOCKS))


def coefficients(decay, write):
    totals = [decay[0:1]]
    for t in range(1, DRAFT):
        totals.append(totals[-1] * decay[t : t + 1])
    row = lax.broadcasted_iota(jnp.int32, (ROWS, SEQS), 0)
    seq = lax.broadcasted_iota(jnp.int32, (ROWS, SEQS), 1)
    token = row % DRAFT

    def column(rows):
        spread = jnp.zeros((ROWS, SEQS), F32)
        for t in range(DRAFT):
            spread = jnp.where(token == t, jnp.broadcast_to(rows[t], (ROWS, SEQS)), spread)
        return jnp.sum(jnp.where(row // DRAFT == seq, spread, 0.0), axis=1, keepdims=True)

    total = column(totals)
    written = column([write[t : t + 1] for t in range(DRAFT)])
    i = lax.broadcasted_iota(jnp.int32, (ROWS, ROWS), 0)
    j = lax.broadcasted_iota(jnp.int32, (ROWS, ROWS), 1)

    def as_row(col):
        return jnp.sum(jnp.where(i == j, jnp.broadcast_to(col, (ROWS, ROWS)), 0.0), axis=0, keepdims=True)

    kept = (i // DRAFT == j // DRAFT) & (j <= i)
    mix = jnp.where(kept, as_row(written) * (total / as_row(total)), 0.0)
    return total, mix


def stack(ref, out):
    for s in range(SEQS):
        out[DRAFT * s : DRAFT * (s + 1), :] = ref[s].astype(F32)


def position():
    xh, core = lax.axis_index("xh"), lax.axis_index("core")
    return 2 * xh + core, core, xh


def first_kernel(
    q_hbm, k_hbm, v_hbm, decay_hbm, write_hbm, cov_hbm, val_hbm,
    msg, cov, val, q32, k32, values, total_out, mix_out, ck, cq,
    q_in, k_in, v_in, v_across, decay_in, write_in, small_sem, big_sem, val_sem,
):
    me, core, xh = position()
    start = pl.multiple_of(me * PART, PART)
    across = pl.multiple_of((2 * (1 - xh) + 1 - core) * PART, PART)
    ends = [
        (decay_hbm, decay_in),
        (write_hbm, write_in),
        (q_hbm, q_in),
        (k_hbm, k_in),
        (v_hbm.at[:, :, pl.ds(start, PART)], v_in),
        (v_hbm.at[:, :, pl.ds(across, PART)], v_across),
    ]
    small = [pltpu.make_async_copy(a, b, small_sem.at[n]) for n, (a, b) in enumerate(ends)]
    big = [
        [
            pltpu.make_async_copy(
                cov_hbm.at[pl.ds(2 * p, 2), :, pl.ds(PART * b, PART)],
                cov.at[pl.ds(2 * p, 2), b],
                big_sem.at[p, b],
            )
            for b in range(BLOCKS)
        ]
        for p in range(SEQS // 2)
    ]
    big.append([pltpu.make_async_copy(val_hbm, val, val_sem)])
    for c in small[:4] + big[0] + small[4:] + big[1] + big[2] + big[3] + big[4]:
        c.start()
    for c in small[:2]:
        c.wait()
    total, mix = coefficients(decay_in[...], write_in[...])
    total_out[...] = jnp.broadcast_to(total, total_out.shape)
    mix_out[...] = mix
    out_of = (q32, k32, values.at[:, :PART], values.at[:, PART:])
    for c, x, out in zip(small[2:], (q_in, k_in, v_in, v_across), out_of):
        c.wait()
        stack(x, out)
    keys = k32[...].astype(BF16)
    keys_mine = k32[:, pl.ds(start, PART)].astype(BF16)
    dots = mm(q32[...].astype(BF16), keys, NT)
    base = mm_wide(mix * dots, keys_mine)
    first = lax.broadcasted_iota(jnp.int32, (8, 1), 0) < DRAFT

    def by_columns(p, pieces):
        both = jnp.concatenate(pieces, axis=0)
        res = [jnp.concatenate([mm(both, cov[2 * p + n, b]) for b in range(BLOCKS)], axis=1) for n in range(2)]
        z = jnp.where(first, res[0][:8] + res[0][8:], res[1][:8] + res[1][8:])
        msg[8 * p : 8 * p + 8, :DK] = (z * total[8 * p : 8 * p + 8]).astype(BF16)

    held = None
    for p in range(SEQS // 2):
        for c in big[p]:
            c.wait()
        rows = slice(8 * p, 8 * p + 8)
        slab = jnp.concatenate([q32[rows, :].astype(BF16), k32[rows, :].astype(BF16)], axis=0)
        res = [by_rows(slab, cov, 2 * p + n) for n in range(2)]
        ck[rows, :] = jnp.where(first, res[0][8:], res[1][8:])
        part = jnp.where(first, res[0][:8], res[1][:8]) * total[rows]
        cq[rows, :] = part
        y = part + base[rows]
        pieces = halves(y)
        msg[8 * p : 8 * p + 8, DK : DK + PART] = pieces[0]
        msg[8 * p : 8 * p + 8, DK + PART :] = pieces[1]
        if held is not None:
            by_columns(*held)
        held = (p, pieces)
    by_columns(*held)
    big[4][0].wait()


def second_kernel(
    ridge, gathered, cov, val, q32, k32, values_in, total_in, mix_in, ck, cq, sent, lhs, low, share_out,
    p32, c32, y32, w32, low32, d32, x32, ap32, ac32, dm32,
):
    total, shift, mix = total_in[:, :1], ridge[0:1, 0:1], mix_in[...]
    me, core, xh = position()
    mine = pl.ds(pl.multiple_of(me * PART, PART), PART)
    first = lax.broadcasted_iota(jnp.int32, (8, 1), 0) < DRAFT

    def dot(a, b):
        return jnp.sum(a * b, axis=1, keepdims=True)

    def dots_of(a, b):
        res = mm(jnp.concatenate(halves(a), axis=0), b, NT)
        return res[:ROWS] + res[ROWS:]

    for g in range(BLOCKS):
        p32[:, g * PART : (g + 1) * PART] = gathered[g, :, DK : DK + PART].astype(F32) + gathered[
            g, :, DK + PART :
        ].astype(F32)
    keys = k32[...].astype(BF16)
    keys_mine = k32[:, mine].astype(BF16)
    c = gathered[0, :, :DK].astype(F32)
    for g in range(1, BLOCKS):
        c = c + gathered[g, :, :DK].astype(F32)
    c32[...] = c
    coef = mix * dots_of(p32[...], keys)
    for p in range(SEQS // 2):
        rows = slice(8 * p, 8 * p + 8)
        pieces = jnp.concatenate(halves(p32[rows, :]) + halves(c32[rows, :]), axis=0)
        res = [by_rows(pieces, cov, 2 * p + n) for n in range(2)]
        res = [(r[:8] + r[8:16], r[16:24] + r[24:]) for r in res]
        ap32[rows, :] = jnp.where(first, res[0][0], res[1][0]) * total[rows]
        ac32[rows, :] = jnp.where(first, res[0][1], res[1][1]) * total[rows]
        if p == 0:
            low32[...] = mm_wide(coef, keys)
            y32[...] = p32[...] + shift * q32[...]
            w32[...] = c32[...] + low32[...] + shift * (p32[...] + y32[...])
    ck_hi, ck_lo = halves(ck[...])
    state_w = ac32[...] + total * (mm_wide(coef, ck_hi) + mm(coef.astype(BF16), ck_lo))
    state_w = state_w + shift * (2.0 * ap32[...] + shift * cq[...])
    image_w = state_w + mm_wide(mix * dots_of(w32[...], keys), keys_mine) + shift * w32[:, mine]

    q, y, w = q32[...], y32[...], w32[...]
    rr0 = dot(q, q)
    a0 = rr0 / dot(q, y)
    res1 = q - a0 * y
    rr1 = dot(res1, res1)
    b0 = rr1 / rr0
    dir1 = res1 + b0 * q
    image1 = (1.0 + b0) * y - a0 * w
    a1 = rr1 / dot(dir1, image1)
    sol2 = a0 * q + a1 * dir1
    res2 = res1 - a1 * image1
    rr2 = dot(res2, res2)
    b1 = rr2 / rr1
    d32[...] = res2 + b1 * dir1
    x32[...] = sol2
    q, y, p = q32[:, mine], y32[:, mine], p32[:, mine]
    w = ap32[...] + low32[:, mine] + shift * (p + y)
    res1 = q - a0 * y
    dir1 = res1 + b0 * q
    image1 = (1.0 + b0) * y - a0 * w
    dir2 = res1 - a1 * image1 + b1 * dir1
    dm32[...] = dir2
    image2 = y - a0 * w - a1 * ((1.0 + b0) * w - a0 * image_w) + b1 * image1
    known = d32[:, mine]
    share = jnp.broadcast_to(dot(known, image2) / rr2, (ROWS, 64))
    missed = mix * mm((dir2 - known).astype(BF16), keys_mine, NT)
    share = jnp.concatenate([share, missed, jnp.zeros((ROWS, 32), F32)], axis=1)
    share_out[...] = share
    for p in range(SEQS // 2):
        rows = slice(8 * p, 8 * p + 8)
        both = [x32[rows, mine].astype(BF16), dm32[rows, :].astype(BF16)]
        lhs[2 * 8 * p : 2 * 8 * (p + 1), :] = jnp.concatenate(both, axis=0)
        if p == 2:
            dots = mm(jnp.concatenate(halves(x32[...]) + (d32[...].astype(BF16),), axis=0), keys, NT)
        by_values(lhs, val, total, xh, 1 - core, p, sent)
    sent[:, SHARE:] = share.astype(BF16)
    values = values_in[:, :PART].astype(BF16)
    low[:, :PART] = mm_wide(mix * (dots[:ROWS] + dots[ROWS : 2 * ROWS]), values)
    low[:, PART:] = mm_wide(mix * dots[2 * ROWS :], values)


def by_values(lhs, val, total, xh, core, p, out):
    rows = slice(8 * p, 8 * p + 8)
    first = lax.broadcasted_iota(jnp.int32, (8, 1), 0) < DRAFT
    both = lhs[16 * p : 16 * p + 16, :]
    for slot, part in enumerate((2 * xh + core, 2 * (1 - xh) + 1 - core)):
        entries = pl.ds(pl.multiple_of(part * PART, PART), PART)
        res = [mm(both, val[2 * p + n, entries, :], NT) for n in range(2)]
        for m in range(2):
            half = slice(8 * m, 8 * m + 8)
            part = jnp.where(first, res[0][half], res[1][half]) * total[rows]
            at = slot * SLOT + m * PART
            out[rows, at : at + PART] = part.astype(out.dtype)


def own_kernel(val, lhs, total_in, low, share, kept):
    _, core, xh = position()
    total = total_in[:, :1]
    for p in range(SEQS // 2):
        by_values(lhs, val, total, xh, core, p, kept)
    kept[:, SHARE:] = share[...]
    kept[:, : 2 * PART] += low[...]


def project(scaled, weight, core, out):
    step = 512
    for x in range(2):
        for n in range(2048 // step):
            cols = pl.ds(pl.multiple_of((2 * x + core) * 2048 + n * step, step), step)
            part = mm(scaled, weight[:, cols])
            for m in range(step // 128):
                out[16 * x + n * (step // 128) + m] = part[:, 128 * m : 128 * (m + 1)].astype(out.dtype)


def third_kernel(mine, partner, arrived, values, gain, weight, sent, scaled, squares):
    pair = mine[...] + partner[...].astype(F32)
    other = arrived[...].astype(F32)
    total = [pair[:, SLOT * n : SLOT * (n + 1)] + other[:, SLOT * (1 - n) : SLOT * (2 - n)] for n in range(2)]
    share = pair[:, SHARE:] + other[:, SHARE:]
    a2 = 1.0 / share[:, :1]
    missed = mm(share[:, 64:96].astype(BF16), values[...].astype(BF16))
    readout = [
        total[n][:, :PART] + a2 * (total[n][:, PART:] + missed[:, PART * n : PART * (n + 1)]) for n in range(2)
    ]
    scaled[...] = (readout[0] * gain[...]).astype(BF16)
    project(scaled[...], weight, 1 - position()[1], sent)
    both = readout[0] * readout[0] + readout[1] * readout[1]
    squares[...] = jnp.broadcast_to(jnp.sum(both, axis=1, keepdims=True), (ROWS, 128))
    sent[32], sent[33] = halves(squares[...])


def last_kernel(scaled, weight, kept):
    project(scaled[...], weight, position()[1], kept)


def join_kernel(kept, arrived, squares, out):
    sums = squares[...] + arrived[32].astype(F32) + arrived[33].astype(F32)
    scale = lax.rsqrt(sums * (1.0 / DV) + 1e-06)
    for n in range(32):
        out[n] = ((kept[n] + arrived[n].astype(F32)) * scale).astype(BF16)


def swapped(x, axis):
    return lax.ppermute(x, axis, [(0, 1), (1, 0)])


def params(mib):
    return pltpu.CompilerParams(vmem_limit_bytes=mib << 20)


def body(
    new_queries, new_keys, new_values, decay_gate, write_gate,
    ridge_shift, norm_gain, cov_state, value_state, out_weight,
):
    q, k, v = (x[:, 0] for x in (new_queries, new_keys, new_values))
    decay, write = (x[:, 0].T for x in (decay_gate, write_gate))
    cov, val, weight = cov_state[:, 0], value_state[:, 0], out_weight[0]

    estimate = pl.CostEstimate(flops=1 << 28, bytes_accessed=1 << 21, transcendentals=0)
    in_hbm = [
        pltpu.with_memory_space_constraint(x, pltpu.HBM)
        for x in (q, k, v, decay, write, cov, val)
    ]
    msg, *carried = pl.pallas_call(
        first_kernel,
        name="first",
        out_shape=(
            pltpu.VMEM((ROWS, DK + 2 * PART), BF16),
            pltpu.VMEM((SEQS, BLOCKS, PART, PART), BF16),
            pltpu.VMEM((SEQS, DV, PART), BF16),
            pltpu.VMEM((ROWS, DK), F32),
            pltpu.VMEM((ROWS, DK), F32),
            pltpu.VMEM((ROWS, SLOT), F32),
            pltpu.VMEM((ROWS, 128), F32),
            pltpu.VMEM((ROWS, ROWS), F32),
            pltpu.VMEM((ROWS, PART), F32),
            pltpu.VMEM((ROWS, PART), F32),
        ),
        in_specs=[HBM] * 7,
        out_specs=(VMEM,) * 10,
        scratch_shapes=[
            pltpu.VMEM((SEQS, DRAFT, DK), BF16),
            pltpu.VMEM((SEQS, DRAFT, DK), BF16),
            pltpu.VMEM((SEQS, DRAFT, PART), BF16),
            pltpu.VMEM((SEQS, DRAFT, PART), BF16),
            pltpu.VMEM((DRAFT, SEQS), F32),
            pltpu.VMEM((DRAFT, SEQS), F32),
            pltpu.SemaphoreType.DMA((6,)),
            pltpu.SemaphoreType.DMA((SEQS // 2, BLOCKS)),
            pltpu.SemaphoreType.DMA,
        ],
        compiler_params=params(16),
    )(*in_hbm)
    gathered = lax.all_gather(msg, KEY)
    sent, lhs, low, share = pl.pallas_call(
        second_kernel,
        name="second",
        out_shape=(
            pltpu.VMEM((ROWS, SHARE + 128), BF16),
            pltpu.VMEM((2 * ROWS, PART), BF16),
            pltpu.VMEM((ROWS, 2 * PART), F32),
            pltpu.VMEM((ROWS, 128), F32),
        ),
        in_specs=[VMEM] * 11,
        out_specs=(VMEM,) * 4,
        scratch_shapes=[pltpu.VMEM((ROWS, n), F32) for n in [DK] * 7 + [PART] * 3],
        compiler_params=params(16),
    )(jnp.broadcast_to(ridge_shift[None], (8, 128)), gathered, *carried)
    kept = pl.pallas_call(
        own_kernel,
        name="own",
        out_shape=pltpu.VMEM((ROWS, SHARE + 128), F32),
        in_specs=[VMEM] * 5,
        out_specs=VMEM,
        compiler_params=params(16),
        cost_estimate=estimate,
    )(carried[1], lhs, carried[5], low, share)
    partner = swapped(sent, "core")
    pair = (kept + partner.astype(F32)).astype(BF16)
    other = lax.ppermute(pair, KEY, [(n, n ^ 3) for n in range(4)])
    sent, scaled, squares = pl.pallas_call(
        third_kernel,
        name="third",
        out_shape=(
            pltpu.VMEM((34, ROWS, 128), BF16),
            pltpu.VMEM((ROWS, PART), BF16),
            pltpu.VMEM((ROWS, 128), F32),
        ),
        in_specs=[VMEM] * 6,
        out_specs=(VMEM,) * 3,
        compiler_params=params(16),
    )(kept, partner, other, carried[4], norm_gain, weight)
    part = pl.pallas_call(
        last_kernel,
        name="last",
        out_shape=pltpu.VMEM((32, ROWS, 128), F32),
        in_specs=[VMEM] * 2,
        out_specs=VMEM,
        compiler_params=params(16),
        cost_estimate=estimate,
    )(scaled, weight)
    part = pl.pallas_call(
        join_kernel,
        name="join",
        out_shape=pltpu.VMEM((32, ROWS, 128), BF16),
        in_specs=[VMEM] * 3,
        out_specs=VMEM,
        compiler_params=params(16),
    )(part, swapped(sent, "core"), squares)
    landed = lax.all_to_all(part, ("xh", "head"), 0, 0, tiled=True)
    return landed.astype(F32).sum(axis=0).astype(BF16).reshape(SEQS, DRAFT, 128)


def solution(mesh):
    fine = Mesh(mesh.devices.reshape(2, 2, *mesh.devices.shape[1:]), ("xh", "core", "head", "batch"))
    placed = (
        P("batch", "head", None, None),
        P("batch", "head", None, None),
        P("batch", "head", None, None),
        P("batch", "head", None),
        P("batch", "head", None),
        P("head"),
        P("head", KEY),
        P("batch", "head", KEY, None),
        P("batch", "head", None, KEY),
        P("head", KEY, None),
    )
    return jax.shard_map(
        body,
        mesh=fine,
        in_specs=placed,
        out_specs=P("batch", None, ("xh", "core", "head")),
        check_vma=False,
    )
```

```python
import jax
import jax.numpy as jnp
from jax import lax
from jax.experimental import pallas as pl
from jax.experimental.pallas import tpu as pltpu
from jax.sharding import Mesh, PartitionSpec as P

DRAFT = 4
SEQS = 8
ROWS = SEQS * DRAFT
DK = 1024
DV = 1024
PART = 256
BLOCKS = DK // PART
SLOT = 2 * PART
SHARE = 2 * SLOT
F32 = jnp.float32
BF16 = jnp.bfloat16
KEY = ("xh", "core")
HBM = pl.BlockSpec(memory_space=pltpu.HBM)
VMEM = pl.BlockSpec(memory_space=pltpu.VMEM)
NT = (((1,), (1,)), ((), ()))
NN = (((1,), (0,)), ((), ()))


def mm(a, b, dims=NN):
    return lax.dot_general(a, b, dims, preferred_element_type=F32)


def halves(x):
    hi = x.astype(BF16)
    return hi, (x - hi.astype(F32)).astype(BF16)


def mm_wide(a, b):
    hi, lo = halves(a)
    return mm(hi, b) + mm(lo, b)


def by_rows(a, cov, s):
    return sum(mm(a[:, PART * b : PART * (b + 1)], cov[s, b], NT) for b in range(BLOCKS))


def coefficients(decay, write):
    totals = [decay[0:1]]
    for t in range(1, DRAFT):
        totals.append(totals[-1] * decay[t : t + 1])
    row = lax.broadcasted_iota(jnp.int32, (ROWS, SEQS), 0)
    seq = lax.broadcasted_iota(jnp.int32, (ROWS, SEQS), 1)
    token = row % DRAFT

    def column(rows):
        spread = jnp.zeros((ROWS, SEQS), F32)
        for t in range(DRAFT):
            spread = jnp.where(token == t, jnp.broadcast_to(rows[t], (ROWS, SEQS)), spread)
        return jnp.sum(jnp.where(row // DRAFT == seq, spread, 0.0), axis=1, keepdims=True)

    total = column(totals)
    written = column([write[t : t + 1] for t in range(DRAFT)])
    i = lax.broadcasted_iota(jnp.int32, (ROWS, ROWS), 0)
    j = lax.broadcasted_iota(jnp.int32, (ROWS, ROWS), 1)

    def as_row(col):
        return jnp.sum(jnp.where(i == j, jnp.broadcast_to(col, (ROWS, ROWS)), 0.0), axis=0, keepdims=True)

    kept = (i // DRAFT == j // DRAFT) & (j <= i)
    mix = jnp.where(kept, as_row(written) * (total / as_row(total)), 0.0)
    return total, mix


def stack(ref, out):
    for s in range(SEQS):
        out[DRAFT * s : DRAFT * (s + 1), :] = ref[s].astype(F32)


def position():
    xh, core = lax.axis_index("xh"), lax.axis_index("core")
    return 2 * xh + core, core, xh


def first_kernel(
    q_hbm, k_hbm, v_hbm, decay_hbm, write_hbm, cov_hbm, val_hbm,
    msg, cov, val, q32, k32, values, total_out, mix_out, ck, cq,
    q_in, k_in, v_in, v_across, decay_in, write_in, small_sem, big_sem, val_sem,
):
    me, core, xh = position()
    start = pl.multiple_of(me * PART, PART)
    across = pl.multiple_of((2 * (1 - xh) + 1 - core) * PART, PART)
    ends = [
        (decay_hbm, decay_in),
        (write_hbm, write_in),
        (q_hbm, q_in),
        (k_hbm, k_in),
        (v_hbm.at[:, :, pl.ds(start, PART)], v_in),
        (v_hbm.at[:, :, pl.ds(across, PART)], v_across),
    ]
    small = [pltpu.make_async_copy(a, b, small_sem.at[n]) for n, (a, b) in enumerate(ends)]
    big = [
        [
            pltpu.make_async_copy(
                cov_hbm.at[pl.ds(2 * p, 2), :, pl.ds(PART * b, PART)],
                cov.at[pl.ds(2 * p, 2), b],
                big_sem.at[p, b],
            )
            for b in range(BLOCKS)
        ]
        for p in range(SEQS // 2)
    ]
    big.append([pltpu.make_async_copy(val_hbm, val, val_sem)])
    for c in small[:4] + big[0] + small[4:] + big[1] + big[2] + big[3] + big[4]:
        c.start()
    for c in small[:2]:
        c.wait()
    total, mix = coefficients(decay_in[...], write_in[...])
    total_out[...] = jnp.broadcast_to(total, total_out.shape)
    mix_out[...] = mix
    out_of = (q32, k32, values.at[:, :PART], values.at[:, PART:])
    for c, x, out in zip(small[2:], (q_in, k_in, v_in, v_across), out_of):
        c.wait()
        stack(x, out)
    keys = k32[...].astype(BF16)
    keys_mine = k32[:, pl.ds(start, PART)].astype(BF16)
    dots = mm(q32[...].astype(BF16), keys, NT)
    base = mm_wide(mix * dots, keys_mine)
    first = lax.broadcasted_iota(jnp.int32, (8, 1), 0) < DRAFT

    def by_columns(p, pieces):
        both = jnp.concatenate(pieces, axis=0)
        res = [jnp.concatenate([mm(both, cov[2 * p + n, b]) for b in range(BLOCKS)], axis=1) for n in range(2)]
        z = jnp.where(first, res[0][:8] + res[0][8:], res[1][:8] + res[1][8:])
        msg[8 * p : 8 * p + 8, :DK] = (z * total[8 * p : 8 * p + 8]).astype(BF16)

    held = None
    for p in range(SEQS // 2):
        for c in big[p]:
            c.wait()
        rows = slice(8 * p, 8 * p + 8)
        slab = jnp.concatenate([q32[rows, :].astype(BF16), k32[rows, :].astype(BF16)], axis=0)
        res = [by_rows(slab, cov, 2 * p + n) for n in range(2)]
        ck[rows, :] = jnp.where(first, res[0][8:], res[1][8:])
        part = jnp.where(first, res[0][:8], res[1][:8]) * total[rows]
        cq[rows, :] = part
        y = part + base[rows]
        pieces = halves(y)
        msg[8 * p : 8 * p + 8, DK : DK + PART] = pieces[0]
        msg[8 * p : 8 * p + 8, DK + PART :] = pieces[1]
        if held is not None:
            by_columns(*held)
        held = (p, pieces)
    by_columns(*held)
    big[4][0].wait()


def second_kernel(
    ridge, gathered, cov, val, q32, k32, values_in, total_in, mix_in, ck, cq, sent, lhs, share_out, d32, x32,
    p32, c32, y32, w32, low32, ap32, ac32, dm32,
):
    total, shift, mix = total_in[:, :1], ridge[0:1, 0:1], mix_in[...]
    me, core, xh = position()
    mine = pl.ds(pl.multiple_of(me * PART, PART), PART)
    first = lax.broadcasted_iota(jnp.int32, (8, 1), 0) < DRAFT

    def dot(a, b):
        return jnp.sum(a * b, axis=1, keepdims=True)

    def dots_of(a, b):
        res = mm(jnp.concatenate(halves(a), axis=0), b, NT)
        return res[:ROWS] + res[ROWS:]

    for g in range(BLOCKS):
        p32[:, g * PART : (g + 1) * PART] = gathered[g, :, DK : DK + PART].astype(F32) + gathered[
            g, :, DK + PART :
        ].astype(F32)
    keys = k32[...].astype(BF16)
    keys_mine = k32[:, mine].astype(BF16)
    c = gathered[0, :, :DK].astype(F32)
    for g in range(1, BLOCKS):
        c = c + gathered[g, :, :DK].astype(F32)
    c32[...] = c
    coef = mix * dots_of(p32[...], keys)
    for p in range(SEQS // 2):
        rows = slice(8 * p, 8 * p + 8)
        pieces = jnp.concatenate(halves(p32[rows, :]) + halves(c32[rows, :]), axis=0)
        res = [by_rows(pieces, cov, 2 * p + n) for n in range(2)]
        res = [(r[:8] + r[8:16], r[16:24] + r[24:]) for r in res]
        ap32[rows, :] = jnp.where(first, res[0][0], res[1][0]) * total[rows]
        ac32[rows, :] = jnp.where(first, res[0][1], res[1][1]) * total[rows]
        if p == 0:
            low32[...] = mm_wide(coef, keys)
            y32[...] = p32[...] + shift * q32[...]
            w32[...] = c32[...] + low32[...] + shift * (p32[...] + y32[...])
    ck_hi, ck_lo = halves(ck[...])
    state_w = ac32[...] + total * (mm_wide(coef, ck_hi) + mm(coef.astype(BF16), ck_lo))
    state_w = state_w + shift * (2.0 * ap32[...] + shift * cq[...])
    image_w = state_w + mm_wide(mix * dots_of(w32[...], keys), keys_mine) + shift * w32[:, mine]

    q, y, w = q32[...], y32[...], w32[...]
    rr0 = dot(q, q)
    a0 = rr0 / dot(q, y)
    res1 = q - a0 * y
    rr1 = dot(res1, res1)
    b0 = rr1 / rr0
    dir1 = res1 + b0 * q
    image1 = (1.0 + b0) * y - a0 * w
    a1 = rr1 / dot(dir1, image1)
    sol2 = a0 * q + a1 * dir1
    res2 = res1 - a1 * image1
    rr2 = dot(res2, res2)
    b1 = rr2 / rr1
    d32[...] = res2 + b1 * dir1
    x32[...] = sol2
    q, y, p = q32[:, mine], y32[:, mine], p32[:, mine]
    w = ap32[...] + low32[:, mine] + shift * (p + y)
    res1 = q - a0 * y
    dir1 = res1 + b0 * q
    image1 = (1.0 + b0) * y - a0 * w
    dir2 = res1 - a1 * image1 + b1 * dir1
    dm32[...] = dir2
    image2 = y - a0 * w - a1 * ((1.0 + b0) * w - a0 * image_w) + b1 * image1
    known = d32[:, mine]
    share = jnp.broadcast_to(dot(known, image2) / rr2, (ROWS, 64))
    missed = mix * mm((dir2 - known).astype(BF16), keys_mine, NT)
    share = jnp.concatenate([share, missed, jnp.zeros((ROWS, 32), F32)], axis=1)
    share_out[...] = share
    for p in range(SEQS // 2):
        rows = slice(8 * p, 8 * p + 8)
        both = [x32[rows, mine].astype(BF16), dm32[rows, :].astype(BF16)]
        lhs[2 * 8 * p : 2 * 8 * (p + 1), :] = jnp.concatenate(both, axis=0)
        by_values(lhs, val, total, xh, 1 - core, p, sent)
    sent[:, SHARE:] = share.astype(BF16)


def by_values(lhs, val, total, xh, core, p, out):
    rows = slice(8 * p, 8 * p + 8)
    first = lax.broadcasted_iota(jnp.int32, (8, 1), 0) < DRAFT
    both = lhs[16 * p : 16 * p + 16, :]
    for slot, part in enumerate((2 * xh + core, 2 * (1 - xh) + 1 - core)):
        entries = pl.ds(pl.multiple_of(part * PART, PART), PART)
        res = [mm(both, val[2 * p + n, entries, :], NT) for n in range(2)]
        for m in range(2):
            half = slice(8 * m, 8 * m + 8)
            part = jnp.where(first, res[0][half], res[1][half]) * total[rows]
            at = slot * SLOT + m * PART
            out[rows, at : at + PART] = part.astype(out.dtype)


def own_kernel(val, lhs, total_in, mix_in, values_in, k32, share, d32, x32, kept):
    _, core, xh = position()
    total, mix = total_in[:, :1], mix_in[...]
    keys, values = k32[...].astype(BF16), values_in[:, :PART].astype(BF16)
    dots = mm(jnp.concatenate(halves(x32[...]) + (d32[...].astype(BF16),), axis=0), keys, NT)
    for p in range(SEQS // 2):
        by_values(lhs, val, total, xh, core, p, kept)
        if p == 1:
            low = [mm_wide(mix * (dots[:ROWS] + dots[ROWS : 2 * ROWS]), values)]
            low.append(mm_wide(mix * dots[2 * ROWS :], values))
    kept[:, SHARE:] = share[...]
    for m in range(2):
        kept[:, m * PART : (m + 1) * PART] += low[m]


def project(scaled, weight, core, out):
    step = 512
    for x in range(2):
        for n in range(2048 // step):
            cols = pl.ds(pl.multiple_of((2 * x + core) * 2048 + n * step, step), step)
            part = mm(scaled, weight[:, cols])
            for m in range(step // 128):
                out[16 * x + n * (step // 128) + m] = part[:, 128 * m : 128 * (m + 1)].astype(out.dtype)


def third_kernel(mine, partner, arrived, values, gain, weight, sent, scaled, squares):
    pair = mine[...] + partner[...].astype(F32)
    other = arrived[...].astype(F32)
    total = [pair[:, SLOT * n : SLOT * (n + 1)] + other[:, SLOT * (1 - n) : SLOT * (2 - n)] for n in range(2)]
    share = pair[:, SHARE:] + other[:, SHARE:]
    a2 = 1.0 / share[:, :1]
    missed = mm(share[:, 64:96].astype(BF16), values[...].astype(BF16))
    readout = [
        total[n][:, :PART] + a2 * (total[n][:, PART:] + missed[:, PART * n : PART * (n + 1)]) for n in range(2)
    ]
    scaled[...] = (readout[0] * gain[...]).astype(BF16)
    project(scaled[...], weight, 1 - position()[1], sent)
    both = readout[0] * readout[0] + readout[1] * readout[1]
    squares[...] = jnp.broadcast_to(jnp.sum(both, axis=1, keepdims=True), (ROWS, 128))
    sent[32], sent[33] = halves(squares[...])


def last_kernel(scaled, weight, kept):
    project(scaled[...], weight, position()[1], kept)


def join_kernel(kept, arrived, squares, out):
    sums = squares[...] + arrived[32].astype(F32) + arrived[33].astype(F32)
    scale = lax.rsqrt(sums * (1.0 / DV) + 1e-06)
    for n in range(32):
        out[n] = ((kept[n] + arrived[n].astype(F32)) * scale).astype(BF16)


def swapped(x, axis):
    return lax.ppermute(x, axis, [(0, 1), (1, 0)])


def params(mib):
    return pltpu.CompilerParams(vmem_limit_bytes=mib << 20)


def body(
    new_queries, new_keys, new_values, decay_gate, write_gate,
    ridge_shift, norm_gain, cov_state, value_state, out_weight,
):
    q, k, v = (x[:, 0] for x in (new_queries, new_keys, new_values))
    decay, write = (x[:, 0].T for x in (decay_gate, write_gate))
    cov, val, weight = cov_state[:, 0], value_state[:, 0], out_weight[0]

    estimate = pl.CostEstimate(flops=1 << 28, bytes_accessed=1 << 21, transcendentals=0)
    in_hbm = [
        pltpu.with_memory_space_constraint(x, pltpu.HBM)
        for x in (q, k, v, decay, write, cov, val)
    ]
    msg, *carried = pl.pallas_call(
        first_kernel,
        name="first",
        out_shape=(
            pltpu.VMEM((ROWS, DK + 2 * PART), BF16),
            pltpu.VMEM((SEQS, BLOCKS, PART, PART), BF16),
            pltpu.VMEM((SEQS, DV, PART), BF16),
            pltpu.VMEM((ROWS, DK), F32),
            pltpu.VMEM((ROWS, DK), F32),
            pltpu.VMEM((ROWS, SLOT), F32),
            pltpu.VMEM((ROWS, 128), F32),
            pltpu.VMEM((ROWS, ROWS), F32),
            pltpu.VMEM((ROWS, PART), F32),
            pltpu.VMEM((ROWS, PART), F32),
        ),
        in_specs=[HBM] * 7,
        out_specs=(VMEM,) * 10,
        scratch_shapes=[
            pltpu.VMEM((SEQS, DRAFT, DK), BF16),
            pltpu.VMEM((SEQS, DRAFT, DK), BF16),
            pltpu.VMEM((SEQS, DRAFT, PART), BF16),
            pltpu.VMEM((SEQS, DRAFT, PART), BF16),
            pltpu.VMEM((DRAFT, SEQS), F32),
            pltpu.VMEM((DRAFT, SEQS), F32),
            pltpu.SemaphoreType.DMA((6,)),
            pltpu.SemaphoreType.DMA((SEQS // 2, BLOCKS)),
            pltpu.SemaphoreType.DMA,
        ],
        compiler_params=params(16),
    )(*in_hbm)
    gathered = lax.all_gather(msg, KEY)
    total, mix = carried[5:7]
    sent, lhs, share, direction, found = pl.pallas_call(
        second_kernel,
        name="second",
        out_shape=(
            pltpu.VMEM((ROWS, SHARE + 128), BF16),
            pltpu.VMEM((2 * ROWS, PART), BF16),
            pltpu.VMEM((ROWS, 128), F32),
            pltpu.VMEM((ROWS, DK), F32),
            pltpu.VMEM((ROWS, DK), F32),
        ),
        in_specs=[VMEM] * 11,
        out_specs=(VMEM,) * 5,
        scratch_shapes=[pltpu.VMEM((ROWS, n), F32) for n in [DK] * 5 + [PART] * 3],
        compiler_params=params(16),
    )(jnp.broadcast_to(ridge_shift[None], (8, 128)), gathered, *carried)
    kept = pl.pallas_call(
        own_kernel,
        name="own",
        out_shape=pltpu.VMEM((ROWS, SHARE + 128), F32),
        in_specs=[VMEM] * 9,
        out_specs=VMEM,
        compiler_params=params(16),
        cost_estimate=estimate,
    )(carried[1], lhs, total, mix, carried[4], carried[3], share, direction, found)
    partner = swapped(sent, "core")
    pair = (kept + partner.astype(F32)).astype(BF16)
    other = lax.ppermute(pair, KEY, [(n, n ^ 3) for n in range(4)])
    sent, scaled, squares = pl.pallas_call(
        third_kernel,
        name="third",
        out_shape=(
            pltpu.VMEM((34, ROWS, 128), BF16),
            pltpu.VMEM((ROWS, PART), BF16),
            pltpu.VMEM((ROWS, 128), F32),
        ),
        in_specs=[VMEM] * 6,
        out_specs=(VMEM,) * 3,
        compiler_params=params(16),
    )(kept, partner, other, carried[4], norm_gain, weight)
    part = pl.pallas_call(
        last_kernel,
        name="last",
        out_shape=pltpu.VMEM((32, ROWS, 128), F32),
        in_specs=[VMEM] * 2,
        out_specs=VMEM,
        compiler_params=params(16),
        cost_estimate=estimate,
    )(scaled, weight)
    part = pl.pallas_call(
        join_kernel,
        name="join",
        out_shape=pltpu.VMEM((32, ROWS, 128), BF16),
        in_specs=[VMEM] * 3,
        out_specs=VMEM,
        compiler_params=params(16),
    )(part, swapped(sent, "core"), squares)
    landed = lax.all_to_all(part, ("xh", "head"), 0, 0, tiled=True)
    return landed.astype(F32).sum(axis=0).astype(BF16).reshape(SEQS, DRAFT, 128)


def solution(mesh):
    fine = Mesh(mesh.devices.reshape(2, 2, *mesh.devices.shape[1:]), ("xh", "core", "head", "batch"))
    placed = (
        P("batch", "head", None, None),
        P("batch", "head", None, None),
        P("batch", "head", None, None),
        P("batch", "head", None),
        P("batch", "head", None),
        P("head"),
        P("head", KEY),
        P("batch", "head", KEY, None),
        P("batch", "head", None, KEY),
        P("head", KEY, None),
    )
    return jax.shard_map(
        body,
        mesh=fine,
        in_specs=placed,
        out_specs=P("batch", None, ("xh", "core", "head")),
        check_vma=False,
    )
```
